512 devices in a mesh: grp: 2 (over y), ha: 16 (over z), wa: 8 (over x), ta: 2 (over core).
Axes of the slice: x: 8, y: 2, z: 16, core: 2. Of those that a mesh axis runs over, the one named last changes fastest.
The devices are a block of a 8x8x16 slice.
Arguments:
- frames: bfloat16 [8, 96, 64, 1024], P(('grp', 'ta'), None, 'ha', 'wa'), parts along dimension 0, may hold values from -14 to 14
- cache_in: bfloat16 [4, 96, 64, 1024], P('grp', None, 'ha', 'wa'), parts along dimension 0, may hold values from -4 to 4
- cache_mid: bfloat16 [4, 96, 64, 1024], P('grp', None, 'ha', 'wa'), parts along dimension 0, may hold values from -4 to 4
- gain_in: float32 [96], replicated, may hold values from 0.25 to 1.75
- gain_mid: float32 [96], replicated, may hold values from 0.25 to 1.75
- weight_in: bfloat16 [3, 3, 96, 288], replicated, may hold values from -0.125 to 0.125
- bias_in: float32 [96], replicated, may hold values from -3 to 3
- weight_mid: bfloat16 [3, 3, 96, 288], replicated, may hold values from -0.125 to 0.125
- bias_mid: float32 [96], replicated, may hold values from -3 to 3
- cotangent: bfloat16 [8, 96, 64, 1024], P(('grp', 'ta'), None, 'ha', 'wa'), parts along dimension 0, may hold values from -6 to 6
Outputs:
- decoded: bfloat16 [8, 96, 64, 1024], P(('grp', 'ta'), None, 'ha', 'wa'), parts along dimension 0
- input_grad: float32 [8, 96, 64, 1024], P(('grp', 'ta'), None, 'ha', 'wa'), parts along dimension 0
The draws below stay inside these ranges and needn't reach their ends.
There are 2 independent parts, one for each index of `grp`. The reference program is written for one: setup_inputs(seed, part) draws one part's arguments, and reference() takes and returns one part's arrays. A program takes and returns all parts, laid end to end along the dimension named above; an argument that names none is the same for every part. Nothing has to cross between parts.
All inputs are finite; a program needn't handle non-finite values.
Results may differ from the reference program's by a relative error of at most 0.006.
Values may be sent and summed in bfloat16 or wider, within the bound.
No kernel may reach another device: no remote copies, remote signals or barrier semaphores. Data moves between devices by JAX's collectives and lax.ppermute only.
A program may use at most 64 MiB of HBM per device.

```python
import jax
import jax.numpy as jnp
from jax import lax

C = 96
F = 4
H = 64
W = 1024


def draw_frames(key, part):
    key_base = jax.random.fold_in(key, 11)
    key_scale = jax.random.fold_in(key, 12)
    base = jax.random.truncated_normal(key_base, -4.0, 4.0, (F, C, H, W), jnp.float32)
    scales = jnp.exp(jax.random.uniform(key_scale, (F, 1, H, W), jnp.float32, -1.2, 1.2))
    return (base * scales).astype(jnp.bfloat16)


def steps_of(stream_key, extent, cuts, least, top_value):
    level = 1.0
    for dim, blocks in cuts:
        draws = jax.random.uniform(jax.random.fold_in(jax.random.fold_in(stream_key, 6), dim), (blocks,), jnp.float32, least / len(cuts), top_value / len(cuts))
        level = level * jnp.repeat(jnp.exp(draws), extent[dim] // blocks).reshape((-1,) + (1,) * (len(extent) - 1 - dim))
    return level


def noise(own_key, extent, scale, bound, pieces=(), held_as=jnp.bfloat16):
    array = scale * jax.random.normal(own_key, extent, jnp.float32)
    if pieces:
        array = array * steps_of(own_key, extent, pieces, -0.22, 0.18)
    return jnp.clip(array, -bound, bound).astype(held_as)


def setup_inputs(seed: int = 0, part: int = 0) -> dict:
    seeds = jax.random.split(jax.random.key(seed), 11)
    own_keys = jax.random.split(jax.random.fold_in(seeds[10], part), 11)
    return {
        "frames": draw_frames(jax.random.fold_in(jax.random.fold_in(seeds[10], part), 71), part),
        "cache_in": noise(own_keys[1], (2, C, H, W), 0.7, 4.0, ((2, 16), (3, 8))),
        "cache_mid": noise(own_keys[2], (2, C, H, W), 0.7, 4.0, ((2, 16), (3, 8))),
        "gain_in": jnp.clip(1.0 + 0.15 * jax.random.normal(seeds[3], (C,), jnp.float32), 0.25, 1.75),
        "gain_mid": jnp.clip(1.0 + 0.15 * jax.random.normal(seeds[4], (C,), jnp.float32), 0.25, 1.75),
        "weight_in": noise(seeds[5], (3, 3, C, 3 * C), (27 * C) ** -0.5, 0.125),
        "bias_in": noise(seeds[6], (C,), 0.5, 3.0, (), jnp.float32),
        "weight_mid": noise(seeds[7], (3, 3, C, 3 * C), (27 * C) ** -0.5, 0.125),
        "bias_mid": noise(seeds[8], (C,), 0.5, 3.0, (), jnp.float32),
        "cotangent": noise(own_keys[9], (F, C, H, W), 1.0, 6.0, ((0, 2), (2, 16), (3, 8))),
    }


epsilon = 1e-06

def activate(values, gain):
    values = values.astype(jnp.float32)
    mean_square = lax.optimization_barrier(jnp.mean(values * values, axis=1, keepdims=True))
    scaled = values * lax.rsqrt(mean_square + epsilon) * gain[None, :, None, None]
    return jax.nn.silu(scaled)

def act_back(values, gain, upstream):
    values = values.astype(jnp.float32)
    mean_square = lax.optimization_barrier(jnp.mean(values * values, axis=1, keepdims=True))
    inverse = lax.rsqrt(mean_square + epsilon)
    gains = gain[None, :, None, None]
    scaled = values * inverse * gains
    sigmoid_part = jax.nn.sigmoid(scaled)
    weighted = gains * upstream * sigmoid_part * (1.0 + scaled * (1.0 - sigmoid_part))
    return inverse * weighted - values * inverse ** 3 * lax.optimization_barrier(jnp.mean(weighted * values, axis=1, keepdims=True))

def flipped(weight):
    channels = weight.shape[2]
    five = weight.reshape(3, 3, channels, 3, channels)[::-1, ::-1, :, ::-1, :]
    return jnp.transpose(five, (0, 1, 4, 3, 2)).reshape(3, 3, channels, 3 * channels)

def pad_grid(values):
    return jnp.pad(values, ((0, 0), (0, 0), (1, 1), (1, 1)))

def convolve(padded, weight):
    count_frames = padded.shape[0] - 2
    height = padded.shape[2] - 2
    width = padded.shape[3] - 2
    weights = weight.astype(jnp.float32)

    def one_frame(index_frame):
        parts = [lax.dynamic_slice_in_dim(padded, index_frame + time_tap, 1, 0)[0] for time_tap in range(3)]
        stacked = jnp.concatenate(parts, 0).astype(jnp.float32)
        summed = jnp.zeros((weight.shape[2], height, width), jnp.float32)
        for row_tap in range(3):
            for col_tap in range(3):
                summed = summed + jnp.einsum('ok,khw->ohw', weights[row_tap, col_tap], stacked[:, row_tap:row_tap + height, col_tap:col_tap + width])
        return summed
    return lax.map(one_frame, jnp.arange(count_frames, dtype=jnp.int32))

def reference(frames, cache_in, cache_mid, gain_in, gain_mid, weight_in, bias_in, weight_mid, bias_mid, cotangent):
    active_in = activate(frames, gain_in).astype(jnp.bfloat16)
    padded_in = pad_grid(jnp.concatenate([cache_in, active_in], 0))
    hidden = (convolve(padded_in, weight_in) + bias_in[None, :, None, None]).astype(jnp.bfloat16)
    active_mid = activate(hidden, gain_mid).astype(jnp.bfloat16)
    padded_mid = pad_grid(jnp.concatenate([cache_mid, active_mid], 0))
    residual = convolve(padded_mid, weight_mid) + bias_mid[None, :, None, None]
    decoded = (frames.astype(jnp.float32) + residual).astype(jnp.bfloat16)
    no_frames = jnp.zeros((2,) + cotangent.shape[1:], jnp.bfloat16)
    back_mid = convolve(pad_grid(jnp.concatenate([cotangent, no_frames], 0)), flipped(weight_mid))
    d_hidden = act_back(hidden, gain_mid, back_mid).astype(jnp.bfloat16)
    back_in = convolve(pad_grid(jnp.concatenate([d_hidden, no_frames], 0)), flipped(weight_in))
    input_grad = cotangent.astype(jnp.float32) + act_back(frames, gain_in, back_in)
    return (decoded, input_grad)
```

```python
import jax
import jax.numpy as jnp
from jax import lax
from jax.experimental import pallas as pl
from jax.experimental.pallas import tpu as pltpu
from jax.sharding import PartitionSpec as P

epsilon = 1e-06
f32 = jnp.float32
bf16 = jnp.bfloat16


def lanes_of(shape):
    return lax.broadcasted_iota(jnp.int32, shape, len(shape) - 1)


def act(v, g):
    r = lax.rsqrt(jnp.mean(v * v, axis=0, keepdims=True) + epsilon)
    z = v * r * g
    return z * jax.nn.sigmoid(z)


def act_and_back(v, g, d):
    r = lax.rsqrt(jnp.mean(v * v, axis=0, keepdims=True) + epsilon)
    vr = v * r
    z = vr * g
    s = jax.nn.sigmoid(z)
    q = g * d * s * (1.0 + z * (1.0 - s))
    back = r * q - vr * (r * r) * jnp.mean(q * v, axis=0, keepdims=True)
    return z * s, back


def pack_body(fr, ct, ci, cm, m1, m2, oc, sw, ed, scr):
    channels = m1.shape[1]
    rows = 4
    flat = channels * rows
    ta = lax.axis_index("ta")
    sources = [
        fr[0:flat, :], fr[flat:, :], ct[0:flat, :], ct[flat:, :],
        ci[pl.ds(ta * flat, flat), :], cm[pl.ds(ta * flat, flat), :],
        ci[pl.ds((1 - ta) * flat, flat), :], cm[pl.ds((1 - ta) * flat, flat), :],
    ]
    for s, source in enumerate(sources):
        scr[s] = source.astype(f32)
    k = lax.broadcasted_iota(jnp.int32, (rows * 128, 128), 0)
    j = lanes_of((rows * 128, 128))
    column = jnp.where(j % 4 == 0, 1, jnp.where(j % 4 == 1, 0, jnp.where(j % 4 == 2, 127, 126)))
    chosen = (j < 4 * rows) & (k // 128 == j // 4) & (k % 128 == column)
    chosen = jnp.where(chosen, 1.0, 0.0).astype(bf16)
    edges = jnp.zeros((channels, 128), f32)
    for s in range(6):
        tiles = [scr[s, pl.ds(r, channels, stride=rows), :].astype(bf16) for r in range(rows)]
        part = jnp.dot(jnp.concatenate(tiles, axis=1), chosen, preferred_element_type=f32)
        edges = edges + (pltpu.roll(part, 4 * rows * s, 1) if s else part)

        @pl.when(ta == 0)
        def _():
            for i in range(2):
                m1[2 * s + i] = tiles[2 + i]
                m2[2 * s + i] = tiles[i]
                if s < 4:
                    sw[2 * s + i] = tiles[2 + i]
                    sw[8 + 2 * s + i] = tiles[i]

        @pl.when(ta == 1)
        def _():
            for i in range(2):
                m1[2 * s + i] = tiles[i]
                m2[2 * s + i] = tiles[2 + i]
                if s < 4:
                    sw[2 * s + i] = tiles[i]
                    sw[8 + 2 * s + i] = tiles[2 + i]

    for s in range(2):
        for r in range(rows):
            oc[s, r] = scr[6 + s, pl.ds(r, channels, stride=rows), :].astype(bf16)
    ed[...] = edges.astype(bf16)


def main_body(
    m1, m2, oc, sp, z1, z2, w1, w2, w1f, w2f, vec, keep, send,
    A, C, M, D, HID, PA, PC, EA, EC,
):
    channels = m1.shape[1]
    tile = (channels, 128)
    ta = lax.axis_index("ta")
    ha = lax.axis_index("ha")
    wa = lax.axis_index("wa")
    first_row = (ta == 1) | (ha > 0)
    last_row = (ta == 0) | (ha < lax.axis_size("ha") - 1)
    left_col = wa > 0
    right_col = wa < lax.axis_size("wa") - 1
    other = 1 - ta
    zb = 4 * ta
    mb = 4 - 4 * ta
    lane = lanes_of(tile)
    column = lane % 4
    gin = jnp.broadcast_to(vec[:, 0:1], tile)
    gmid = jnp.broadcast_to(vec[:, 1:2], tile)
    bin_ = jnp.broadcast_to(vec[:, 2:3], tile)
    bmid = jnp.broadcast_to(vec[:, 3:4], tile)
    zero = jnp.zeros(tile, bf16)

    for i in range(2):
        for r in range(2):
            for src, at, frame, row in (
                (m2, 2 * i + r, 2 * ta + i, 2 + r),
                (m1, 2 * i + r, 2 * ta + i, mb + r),
                (z1, 2 * i + r, 2 * ta + i, zb + r),
                (sp, 2 * i + r, 2 * other + i, 2 + r),
                (sp, 8 + 2 * i + r, 2 * other + i, mb + r),
                (z2, 2 * i + r, 2 * other + i, zb + r),
            ):
                A[2 + frame, row] = act(src[at].astype(f32), gin).astype(bf16)
                C[frame, row] = src[at + 4]
    for r in range(2):
        A[ta, 2 + r] = m2[8 + r]
        A[ta, mb + r] = m1[8 + r]
        A[ta, zb + r] = z1[8 + r]
        A[other, zb + r] = z2[8 + r]
        M[ta, 1 + r] = m2[10 + r]
    M[ta, 3 - 3 * ta] = m1[10 + ta]
    M[ta, 3 * ta] = z1[11 - ta]
    M[other, 3 * ta] = z2[11 - ta]
    for r in range(4):
        A[other, r + 2 - 2 * ta] = oc[0, r]
    for k in range(3):
        M[other, k + 1 - ta] = oc[1, k + ta]
    for e in range(6):
        C[4, e] = zero
        C[5, e] = zero
    for e in range(4):
        D[4, e] = zero
        D[5, e] = zero

    own, par, zo, zp = (t[...].astype(f32) for t in (m2.at[12], sp.at[16], z1.at[12], z2.at[12]))

    def placed(t, slot, start, rows_from, rows, to):
        moved = pltpu.roll(t, (start + 4 * to - 16 * slot - 4 * rows_from) % 128, 1)
        low = start + 4 * to
        return jnp.where((lane >= low) & (lane < low + 4 * rows), moved, 0.0)

    def group(first, swapped):
        mine = yours = 0.0
        for i in range(2):
            mine += placed(own, first + i, 32 * i, 0, 4, 2 - 2 * ta)
            mine += placed(zo, first + i, 32 * i, 2 - 2 * ta, 2, 4 * ta)
            yours += placed(par, first + i, 32 * i, 0, 4, 2 - 2 * ta)
            yours += placed(zp, first + i, 32 * i, 2 - 2 * ta, 2, 4 * ta)
        g0 = jnp.where(ta == 0, mine, yours)
        g1 = jnp.where(ta == 0, yours, mine)
        return g0 + pltpu.roll(g1, 64, 1)

    def caches(slot):
        out = placed(own, slot, 32 * ta, 0, 4, 2 - 2 * ta)
        out += placed(zo, slot, 32 * ta, 2 - 2 * ta, 2, 4 * ta)
        out += placed(par, slot, 32 * other, 0, 4, 2 - 2 * ta)
        return out + placed(zp, slot, 32 * other, 2 - 2 * ta, 2, 4 * ta)

    def edge_products(w, low, high):
        pieces = []
        for t in range(3):
            for a in range(3):
                s = 32 * t + 4 * a
                if s == 0:
                    pieces.append(low.astype(bf16))
                    continue
                moved = pltpu.roll(low, 128 - s, 1)
                beyond = 0.0 if high is None else pltpu.roll(high, 128 - s, 1)
                pieces.append(jnp.where(lane < 128 - s, moved, beyond).astype(bf16))
        p = jnp.dot(w[...], jnp.concatenate(pieces, axis=0), preferred_element_type=f32)
        p0, p1, p2 = (p[b * channels : (b + 1) * channels] for b in range(3))
        across = jnp.where(column == 2, p0, p2)
        own_part = jnp.where(column == 2, pltpu.roll(p0, 127, 1), pltpu.roll(p2, 1, 1)) + p1
        return across, own_part

    act_edges = pltpu.roll(act(group(0, True), gin), 64, 1)
    cin_edges = caches(4)
    across, own_part = edge_products(
        w1, jnp.where(lane < 64, cin_edges, act_edges), jnp.where(lane < 64, act_edges, 0.0)
    )
    PA[...] = across
    EA[...] = own_part
    across, own_part = edge_products(w2f, group(2, True), None)
    PC[...] = across
    EC[...] = own_part
    cmid_edges = pltpu.roll(caches(5), 124, 1)

    def products(w, ref, f, row):
        cols = []
        for i in range(2):
            cols.append(
                jnp.concatenate(
                    [ref[f + t, row + i + a] for t in range(3) for a in range(3)], axis=0
                )
            )
        p = jnp.dot(w[...], jnp.concatenate(cols, axis=1), preferred_element_type=f32)
        return [
            [p[b * channels : (b + 1) * channels, 128 * i : 128 * (i + 1)] for b in range(3)]
            for i in range(2)
        ]

    def shifted_sum(p, edge_ref, q):
        back = pltpu.roll(edge_ref[...], lax.rem(256 - (q + 2), 128), 1)
        out = p[1] + jnp.where(lane == 0, back, pltpu.roll(p[0], 1, 1))
        return out + jnp.where(lane == 127, back, pltpu.roll(p[2], 127, 1))

    def to_edges(p, edge_ref, q):
        moved = pltpu.roll(jnp.where(lane == 0, p[2], p[0]), q + 2, 1)
        here = (lane == q + 1) | (lane == q + 2)
        edge_ref[...] = edge_ref[...] + jnp.where(here, moved, 0.0)

    def first_layer(f, carry):
        for pair in range(2):
            pf = products(w1, A, f, 2 * pair)
            pb = products(w2f, C, f, 2 * pair)
            for i in range(2):
                e = 2 * pair + i
                q = f * 32 + e * 4
                hidden = (shifted_sum(pf[i], PA, q) + bin_).astype(bf16).astype(f32)
                back = shifted_sum(pb[i], PC, q)
                to_edges(pf[i], EA, q)
                to_edges(pb[i], EC, q)
                a, d = act_and_back(hidden, gmid, back)
                if e == 0:
                    a = jnp.where(first_row, a, 0.0)
                    d = jnp.where(first_row, d, 0.0)
                if e == 3:
                    a = jnp.where(last_row, a, 0.0)
                    d = jnp.where(last_row, d, 0.0)
                M[2 + f, e] = a.astype(bf16)
                D[f, e] = d.astype(bf16)
        return carry

    lax.fori_loop(0, 4, first_layer, 0)

    hidden = (EA[...] + bin_).astype(bf16).astype(f32)
    a, d = act_and_back(hidden, gmid, EC[...])
    row = (lane % 32) // 4
    inside = ((column == 2) & left_col) | ((column == 1) & right_col)
    inside = inside & (row < 4) & ((row > 0) | first_row) & ((row < 3) | last_row)
    a = jnp.where(inside, a, 0.0).astype(bf16).astype(f32)
    d = jnp.where(inside, d, 0.0).astype(bf16).astype(f32)
    a = pltpu.roll(a, 64, 1)
    low = jnp.where(lane < 64, cmid_edges, a)
    across, _ = edge_products(w2, low, jnp.where(lane < 64, a, 0.0))
    PA[...] = across
    across, _ = edge_products(w1f, d, None)
    PC[...] = across

    def second_layer(f, mine, slot):
        pf = products(w2, M, f, 0)
        pb = products(w1f, D, f, 0)
        for i in range(2):
            q = f * 32 + i * 4
            frame = mine[2 * slot + i].astype(f32)
            cot = mine[4 + 2 * slot + i].astype(f32)
            decoded = frame + (shifted_sum(pf[i], PA, q) + bmid)
            _, back = act_and_back(frame, gin, shifted_sum(pb[i], PC, q))
            yield i, decoded.astype(bf16).astype(f32), cot + back

    def second(slot, carry):
        for i, decoded, grad in second_layer(2 * ta + slot, m2, slot):
            keep[0, slot, i] = decoded
            keep[1, slot, i] = grad
        for i, decoded, grad in second_layer(2 * other + slot, sp, slot):
            send[0, slot, i] = decoded
            send[1, slot, i] = grad
        return carry

    lax.fori_loop(0, 2, second, 0)


def assemble_body(keep, got, dec, grad, scr):
    channels = keep.shape[3]
    flat = 4 * channels
    ta = lax.axis_index("ta")

    def write(at_keep, at_got):
        for f in range(2):
            for i in range(2):
                for src, r in ((keep, at_keep + i), (got, at_got + i)):
                    scr[pl.ds(f * flat + r, channels, stride=4), :] = src[0, f, i]
                    grad[pl.ds(f * flat + r, channels, stride=4), :] = src[1, f, i]

    @pl.when(ta == 0)
    def _():
        write(0, 2)

    @pl.when(ta == 1)
    def _():
        write(2, 0)

    dec[...] = scr[...].astype(bf16)


def forward_weights(weight):
    c = weight.shape[2]
    five = weight.reshape(3, 3, c, 3, c)
    return jnp.transpose(five, (1, 2, 3, 0, 4)).reshape(3 * c, 9 * c)


def flipped_weights(weight):
    c = weight.shape[2]
    five = weight.reshape(3, 3, c, 3, c)[::-1, ::-1, :, ::-1, :]
    return jnp.transpose(five, (1, 4, 3, 0, 2)).reshape(3 * c, 9 * c)


def per_device(
    frames, cache_in, cache_mid, gain_in, gain_mid,
    weight_in, bias_in, weight_mid, bias_mid, cotangent,
):
    n, c, height, width = frames.shape
    flat = lambda v: v.reshape(n * c * height, width)
    tile = (c, width)
    m1, m2, oc, sw, ed = pl.pallas_call(
        pack_body,
        out_shape=(
            jax.ShapeDtypeStruct((13,) + tile, bf16),
            jax.ShapeDtypeStruct((13,) + tile, bf16),
            jax.ShapeDtypeStruct((2, 4) + tile, bf16),
            jax.ShapeDtypeStruct((17,) + tile, bf16),
            jax.ShapeDtypeStruct(tile, bf16),
        ),
        scratch_shapes=[pltpu.VMEM((8, c * height, width), f32)],
        name="pack",
    )(flat(frames), flat(cotangent), flat(cache_in), flat(cache_mid))

    wide = lax.axis_size("wa")
    high = lax.axis_size("ha")
    from_left = lax.ppermute(ed, "wa", [(i, i + 1) for i in range(wide - 1)])
    from_right = lax.ppermute(ed, "wa", [(i + 1, i) for i in range(wide - 1)])
    edge = jnp.where(lanes_of(tile) % 4 >= 2, from_left, from_right)
    m1 = m1.at[12].set(edge)
    m2 = m2.at[12].set(edge)
    sw = sw.at[16].set(edge)
    one = [(2 * i, 2 * i + 2) for i in range(high - 1)]
    one += [(2 * i + 3, 2 * i + 1) for i in range(high - 1)]
    two = [(2 * i + 2, 2 * i + 1) for i in range(high - 1)]
    two += [(2 * i + 1, 2 * i + 2) for i in range(high - 1)]
    z1 = lax.ppermute(m1, ("ha", "ta"), one)
    z2 = lax.ppermute(m2, ("ha", "ta"), two)
    sp = lax.ppermute(sw, "ta", [(0, 1), (1, 0)])

    w1, w2 = forward_weights(weight_in), forward_weights(weight_mid)
    w1f, w2f = flipped_weights(weight_in), flipped_weights(weight_mid)
    vec = jnp.stack([gain_in, gain_mid, bias_in, bias_mid], axis=1)
    half = jax.ShapeDtypeStruct((2, 2, 2) + tile, f32)
    keep, send = pl.pallas_call(
        main_body,
        out_shape=(half, half),
        scratch_shapes=[
            pltpu.VMEM((6, 6) + tile, bf16),
            pltpu.VMEM((6, 6) + tile, bf16),
            pltpu.VMEM((6, 4) + tile, bf16),
            pltpu.VMEM((6, 4) + tile, bf16),
            pltpu.VMEM((4, 4) + tile, bf16),
            pltpu.VMEM(tile, f32),
            pltpu.VMEM(tile, f32),
            pltpu.VMEM(tile, f32),
            pltpu.VMEM(tile, f32),
        ],
        name="block",
    )(m1, m2, oc, sp, z1, z2, w1, w2, w1f, w2f, vec)

    got = lax.ppermute(send, "ta", [(0, 1), (1, 0)])
    decoded, grad = pl.pallas_call(
        assemble_body,
        out_shape=(
            jax.ShapeDtypeStruct((n * c * height, width), bf16),
            jax.ShapeDtypeStruct((n * c * height, width), f32),
        ),
        scratch_shapes=[pltpu.VMEM((n * c * height, width), f32)],
        name="assemble",
    )(keep, got)
    return decoded.reshape(frames.shape), grad.reshape(frames.shape)


def solution(mesh):
    split = P(("grp", "ta"), None, "ha", "wa")
    cache = P("grp", None, "ha", "wa")
    return jax.shard_map(
        per_device,
        mesh=mesh,
        in_specs=(split, cache, cache, P(), P(), P(), P(), P(), P(), split),
        out_specs=(split, split),
        check_vma=False,
    )
```

```python
import jax
import jax.numpy as jnp
from jax import lax
from jax.experimental import pallas as pl
from jax.experimental.pallas import tpu as pltpu
from jax.sharding import PartitionSpec as P

epsilon = 1e-06
f32 = jnp.float32
bf16 = jnp.bfloat16
VM = pl.BlockSpec(memory_space=pltpu.VMEM)
HB = pl.BlockSpec(memory_space=pltpu.HBM)


def near(*values):
    return [pltpu.with_memory_space_constraint(v, pltpu.VMEM) for v in values]


def far(*values):
    return [pltpu.with_memory_space_constraint(v, pltpu.HBM) for v in values]


def lanes_of(shape):
    return lax.broadcasted_iota(jnp.int32, shape, len(shape) - 1)


def act(v, g):
    r = lax.rsqrt(jnp.mean(v * v, axis=0, keepdims=True) + epsilon)
    z = v * r * g
    return z * jax.nn.sigmoid(z)


def act_and_back(v, g, d):
    r = lax.rsqrt(jnp.mean(v * v, axis=0, keepdims=True) + epsilon)
    vr = v * r
    z = vr * g
    s = jax.nn.sigmoid(z)
    q = g * d * s * (1.0 + z * (1.0 - s))
    back = r * q - vr * (r * r) * jnp.mean(q * v, axis=0, keepdims=True)
    return z * s, back


def pack_body(fr_far, ct_far, ci_far, cm_far, m1, m2, oc, sw, ed, scr, inp, sems):
    copies = [
        pltpu.make_async_copy(source, inp.at[i], sems.at[i])
        for i, source in enumerate((fr_far, ct_far, ci_far, cm_far))
    ]
    for copy in copies:
        copy.start()
    channels = m1.shape[1]
    rows = 4
    flat = channels * rows
    ta = lax.axis_index("ta")
    starts = [(0, 0), (0, flat), (1, 0), (1, flat), (2, ta * flat), (3, ta * flat)]
    starts += [(2, (1 - ta) * flat), (3, (1 - ta) * flat)]
    k = lax.broadcasted_iota(jnp.int32, (rows * 128, 128), 0)
    j = lanes_of((rows * 128, 128))
    column = jnp.where(j % 4 == 0, 1, jnp.where(j % 4 == 1, 0, jnp.where(j % 4 == 2, 127, 126)))
    chosen = (j < 4 * rows) & (k // 128 == j // 4) & (k % 128 == column)
    chosen = jnp.where(chosen, 1.0, 0.0).astype(bf16)
    edges = jnp.zeros((channels, 128), f32)
    for s, (array, start) in enumerate(starts):
        if s in (0, 2, 4, 5):
            copies[array].wait()
        scr[s] = inp[array, pl.ds(start, flat), :].astype(f32)
    for s in range(6):
        tiles = [scr[s, pl.ds(r, channels, stride=rows), :].astype(bf16) for r in range(rows)]
        part = jnp.dot(jnp.concatenate(tiles, axis=1), chosen, preferred_element_type=f32)
        edges = edges + (pltpu.roll(part, 4 * rows * s, 1) if s else part)

        @pl.when(ta == 0)
        def _():
            for i in range(2):
                m1[2 * s + i] = tiles[2 + i]
                m2[2 * s + i] = tiles[i]
                if s < 4:
                    sw[2 * s + i] = tiles[2 + i]
                    sw[8 + 2 * s + i] = tiles[i]

        @pl.when(ta == 1)
        def _():
            for i in range(2):
                m1[2 * s + i] = tiles[i]
                m2[2 * s + i] = tiles[2 + i]
                if s < 4:
                    sw[2 * s + i] = tiles[i]
                    sw[8 + 2 * s + i] = tiles[2 + i]

    for s in range(2):
        for r in range(rows):
            oc[s, r] = scr[6 + s, pl.ds(r, channels, stride=rows), :].astype(bf16)
    ed[...] = edges.astype(bf16)


def merge_body(first, second, m1_in, m2_in, sw_in, m1, m2, sw):
    even = lax.rem(lax.axis_index("wa"), 2) == 0
    a, b = first[...].astype(f32), second[...].astype(f32)
    inner = lanes_of(a.shape) % 4 >= 2
    edge = jnp.where(inner == even, b, a).astype(bf16)
    m1[12] = edge
    m2[12] = edge
    sw[16] = edge


def weights_body(
    far_in, far_mid, gi, gm, bi, bm, after, w1, w2, w1f, w2f, vec, win, wmid, sems
):
    copies = [
        pltpu.make_async_copy(far_in, win, sems.at[0]),
        pltpu.make_async_copy(far_mid, wmid, sems.at[1]),
    ]
    for copy in copies:
        copy.start()
    channels = w1.shape[0] // 3
    for k, row in enumerate((gi, gm, bi, bm)):
        vec[k] = jnp.transpose(jnp.broadcast_to(row[...], (128, channels)))
    for copy, src, plain, turned in zip(copies, (win, wmid), (w1, w2), (w1f, w2f)):
        copy.wait()
        plain[...] = jnp.concatenate([src[a].astype(f32) for a in range(3)], axis=1).astype(bf16)
        for b in range(3):
            flat = [
                jnp.transpose(src[2 - a, (2 - b) * channels : (3 - b) * channels, :].astype(f32))
                for a in range(3)
            ]
            blocks = [
                flat[a][(2 - t) * channels : (3 - t) * channels] for t in range(3) for a in range(3)
            ]
            turned[b * channels : (b + 1) * channels, :] = jnp.concatenate(blocks, axis=1).astype(
                bf16
            )


def main_body(
    m1, m2, oc, sp, z1, z2, w1, w2, w1f, w2f, vec, keep, send,
    A, C, M, D, PA, PC, EA, EC,
):
    channels = m1.shape[1]
    tile = (channels, 128)
    ta = lax.axis_index("ta")
    ha = lax.axis_index("ha")
    wa = lax.axis_index("wa")
    first_row = (ta == 1) | (ha > 0)
    last_row = (ta == 0) | (ha < lax.axis_size("ha") - 1)
    left_col = wa > 0
    right_col = wa < lax.axis_size("wa") - 1
    other = 1 - ta
    zb = 4 * ta
    mb = 4 - 4 * ta
    lane = lanes_of(tile)
    column = lane % 4
    gin, gmid, bin_, bmid = (vec[k] for k in range(4))

    for i in range(2):
        for r in range(2):
            for src, at, frame, row in (
                (m2, 2 * i + r, 2 * ta + i, 2 + r),
                (m1, 2 * i + r, 2 * ta + i, mb + r),
                (z1, 2 * i + r, 2 * ta + i, zb + r),
                (sp, 2 * i + r, 2 * other + i, 2 + r),
                (sp, 8 + 2 * i + r, 2 * other + i, mb + r),
                (z2, 2 * i + r, 2 * other + i, zb + r),
            ):
                A[2 + frame, row] = act(src[at].astype(f32), gin).astype(bf16)
                C[frame, row] = src[at + 4]
    for r in range(2):
        A[ta, 2 + r] = m2[8 + r]
        A[ta, mb + r] = m1[8 + r]
        A[ta, zb + r] = z1[8 + r]
        A[other, zb + r] = z2[8 + r]
        M[ta, 1 + r] = m2[10 + r]
    M[ta, 3 - 3 * ta] = m1[10 + ta]
    M[ta, 3 * ta] = z1[11 - ta]
    M[other, 3 * ta] = z2[11 - ta]
    for r in range(4):
        A[other, r + 2 - 2 * ta] = oc[0, r]
    for k in range(3):
        M[other, k + 1 - ta] = oc[1, k + ta]

    for e in range(4):
        D[4, e] = jnp.zeros(tile, bf16)
        D[5, e] = jnp.zeros(tile, bf16)

    own, par, zo, zp = (t[...].astype(f32) for t in (m2.at[12], sp.at[16], z1.at[12], z2.at[12]))

    def placed(t, slot, start, rows_from, rows, to):
        moved = pltpu.roll(t, (start + 4 * to - 16 * slot - 4 * rows_from) % 128, 1)
        low = start + 4 * to
        return jnp.where((lane >= low) & (lane < low + 4 * rows), moved, 0.0)

    def group(first, swapped):
        mine = yours = 0.0
        for i in range(2):
            mine += placed(own, first + i, 32 * i, 0, 4, 2 - 2 * ta)
            mine += placed(zo, first + i, 32 * i, 2 - 2 * ta, 2, 4 * ta)
            yours += placed(par, first + i, 32 * i, 0, 4, 2 - 2 * ta)
            yours += placed(zp, first + i, 32 * i, 2 - 2 * ta, 2, 4 * ta)
        g0 = jnp.where(ta == 0, mine, yours)
        g1 = jnp.where(ta == 0, yours, mine)
        return g0 + pltpu.roll(g1, 64, 1)

    def caches(slot):
        out = placed(own, slot, 32 * ta, 0, 4, 2 - 2 * ta)
        out += placed(zo, slot, 32 * ta, 2 - 2 * ta, 2, 4 * ta)
        out += placed(par, slot, 32 * other, 0, 4, 2 - 2 * ta)
        return out + placed(zp, slot, 32 * other, 2 - 2 * ta, 2, 4 * ta)

    time_first = [(t, a) for t in range(3) for a in range(3)]
    row_first = [(t, a) for a in range(3) for t in range(3)]

    def edge_products(w, low, high, order):
        pieces = []
        for t, a in order:
            s = 32 * t + 4 * a
            if s == 0:
                pieces.append(low.astype(bf16))
                continue
            moved = pltpu.roll(low, 128 - s, 1)
            beyond = 0.0 if high is None else pltpu.roll(high, 128 - s, 1)
            pieces.append(jnp.where(lane < 128 - s, moved, beyond).astype(bf16))
        p = jnp.dot(w[...], jnp.concatenate(pieces, axis=0), preferred_element_type=f32)
        p0, p1, p2 = (p[b * channels : (b + 1) * channels] for b in range(3))
        across = jnp.where(column == 2, p0, p2)
        own_part = jnp.where(column == 2, pltpu.roll(p0, 127, 1), pltpu.roll(p2, 1, 1)) + p1
        return across, own_part

    act_edges = pltpu.roll(act(group(0, True), gin), 64, 1)
    cin_edges = caches(4)
    across, own_part = edge_products(
        w1, jnp.where(lane < 64, cin_edges, act_edges), jnp.where(lane < 64, act_edges, 0.0),
        row_first,
    )
    PA[...] = across
    EA[...] = own_part
    across, own_part = edge_products(w2f, group(2, True), None, time_first)
    PC[...] = across
    EC[...] = own_part
    cmid_edges = pltpu.roll(caches(5), 124, 1)

    def products(w, ref, f, row, order):
        cols = [
            jnp.concatenate([ref[f + t, row + i + a] for t, a in order], axis=0) for i in range(2)
        ]
        weights = w[:, : len(order) * channels]
        p = jnp.dot(weights, jnp.concatenate(cols, axis=1), preferred_element_type=f32)
        return [
            [p[b * channels : (b + 1) * channels, 128 * i : 128 * (i + 1)] for b in range(3)]
            for i in range(2)
        ]

    def shifted_sum(p, edge_ref, q):
        back = pltpu.roll(edge_ref[...], lax.rem(256 - (q + 2), 128) if not isinstance(q, int) else (126 - q) % 128, 1)
        out = p[1] + jnp.where(lane == 0, back, pltpu.roll(p[0], 1, 1))
        return out + jnp.where(lane == 127, back, pltpu.roll(p[2], 127, 1))

    def to_edges(p, edge_ref, q):
        moved = pltpu.roll(jnp.where(lane == 0, p[2], p[0]), q + 2, 1)
        here = (lane == q + 1) | (lane == q + 2)
        edge_ref[...] = edge_ref[...] + jnp.where(here, moved, 0.0)

    def first_layer(f):
        for pair in range(2):
            pf = products(w1, A, f, 2 * pair, row_first)
            pb = products(w2f, C, f, 2 * pair, time_first[: 3 * (4 - f)])
            for i in range(2):
                e = 2 * pair + i
                q = f * 32 + e * 4
                hidden = (shifted_sum(pf[i], PA, q) + bin_).astype(bf16).astype(f32)
                back = shifted_sum(pb[i], PC, q)
                to_edges(pf[i], EA, q)
                to_edges(pb[i], EC, q)
                a, d = act_and_back(hidden, gmid, back)
                if e == 0:
                    a = jnp.where(first_row, a, 0.0)
                    d = jnp.where(first_row, d, 0.0)
                if e == 3:
                    a = jnp.where(last_row, a, 0.0)
                    d = jnp.where(last_row, d, 0.0)
                M[2 + f, e] = a.astype(bf16)
                D[f, e] = d.astype(bf16)

    for f in range(4):
        first_layer(f)

    hidden = (EA[...] + bin_).astype(bf16).astype(f32)
    a, d = act_and_back(hidden, gmid, EC[...])
    row = (lane % 32) // 4
    inside = ((column == 2) & left_col) | ((column == 1) & right_col)
    inside = inside & (row < 4) & ((row > 0) | first_row) & ((row < 3) | last_row)
    a = jnp.where(inside, a, 0.0).astype(bf16).astype(f32)
    d = jnp.where(inside, d, 0.0).astype(bf16).astype(f32)
    a = pltpu.roll(a, 64, 1)
    low = jnp.where(lane < 64, cmid_edges, a)
    across, _ = edge_products(w2, low, jnp.where(lane < 64, a, 0.0), row_first)
    PA[...] = across
    across, _ = edge_products(w1f, d, None, time_first)
    PC[...] = across

    def second_layer(f, mine, slot, out):
        pf = products(w2, M, f, 0, row_first)
        pb = products(w1f, D, f, 0, time_first)
        for i in range(2):
            q = f * 32 + i * 4
            frame = mine[2 * slot + i].astype(f32)
            cot = mine[4 + 2 * slot + i].astype(f32)
            decoded = frame + (shifted_sum(pf[i], PA, q) + bmid)
            out[0, slot, i] = decoded.astype(bf16).astype(f32)
            _, back = act_and_back(frame, gin, shifted_sum(pb[i], PC, q))
            out[1, slot, i] = cot + back

    for slot in range(2):
        second_layer(2 * other + slot, sp, slot, send)
    for slot in range(2):
        second_layer(2 * ta + slot, m2, slot, keep)


def assemble_body(keep, got, dec, grad, scr):
    channels = got.shape[3]
    flat = 4 * channels
    ta = lax.axis_index("ta")

    def write(at_keep, at_got):
        for f in range(2):
            for i in range(2):
                for src, r in ((keep, at_keep + i), (got, at_got + i)):
                    scr[pl.ds(f * flat + r, channels, stride=4), :] = src[0, f, i]
                    grad[pl.ds(f * flat + r, channels, stride=4), :] = src[1, f, i]

    @pl.when(ta == 0)
    def _():
        write(0, 2)

    @pl.when(ta == 1)
    def _():
        write(2, 0)

    dec[...] = scr[...].astype(bf16)


def per_device(
    frames, cache_in, cache_mid, gain_in, gain_mid,
    weight_in, bias_in, weight_mid, bias_mid, cotangent,
):
    n, c, height, width = frames.shape
    flat = lambda v: v.reshape(n * c * height, width)
    tile = (c, width)
    limit = lambda mib: pltpu.CompilerParams(vmem_limit_bytes=mib << 20)
    m1, m2, oc, sw, ed = pl.pallas_call(
        pack_body,
        in_specs=[HB] * 4,
        out_specs=(VM,) * 5,
        out_shape=(
            pltpu.VMEM((13,) + tile, bf16),
            pltpu.VMEM((13,) + tile, bf16),
            pltpu.VMEM((2, 4) + tile, bf16),
            pltpu.VMEM((17,) + tile, bf16),
            pltpu.VMEM(tile, bf16),
        ),
        scratch_shapes=[
            pltpu.VMEM((8, c * height, width), f32),
            pltpu.VMEM((4, n * c * height, width), bf16),
            pltpu.SemaphoreType.DMA((4,)),
        ],
        compiler_params=limit(8),
        name="pack",
    )(*far(flat(frames), flat(cotangent), flat(cache_in), flat(cache_mid)))

    wide = lax.axis_size("wa")
    high = lax.axis_size("ha")
    pairs = lambda start: [
        p for i in range(start, wide - 1, 2) for p in ((i, i + 1), (i + 1, i))
    ]
    first = lax.ppermute(ed, "wa", pairs(0))
    second = lax.ppermute(ed, "wa", pairs(1))
    m1, m2, sw = pl.pallas_call(
        merge_body,
        in_specs=[VM] * 5,
        out_specs=(VM,) * 3,
        out_shape=(
            pltpu.VMEM((13,) + tile, bf16),
            pltpu.VMEM((13,) + tile, bf16),
            pltpu.VMEM((17,) + tile, bf16),
        ),
        input_output_aliases={2: 0, 3: 1, 4: 2},
        compiler_params=limit(2),
        name="merge",
    )(*near(first, second, m1, m2, sw))
    one = [(2 * i, 2 * i + 2) for i in range(high - 1)]
    one += [(2 * i + 3, 2 * i + 1) for i in range(high - 1)]
    two = [(2 * i + 2, 2 * i + 1) for i in range(high - 1)]
    two += [(2 * i + 1, 2 * i + 2) for i in range(high - 1)]
    z1 = lax.ppermute(m1, ("ha", "ta"), one)
    z2 = lax.ppermute(m2, ("ha", "ta"), two)
    sp = lax.ppermute(sw, "ta", [(0, 1), (1, 0)])

    row = lambda v: v.reshape(1, c)
    taps = lambda w: w.reshape(3, 3 * c, 3 * c)
    matrix = pltpu.VMEM((3 * c, 9 * c), bf16)
    w1, w2, w1f, w2f, vec = pl.pallas_call(
        weights_body,
        in_specs=[HB] * 2 + [VM] * 4 + [pl.BlockSpec(memory_space=pl.ANY)],
        out_specs=(VM,) * 5,
        out_shape=(matrix,) * 4 + (pltpu.VMEM((4,) + tile, f32),),
        scratch_shapes=[
            pltpu.VMEM((3, 3 * c, 3 * c), bf16),
            pltpu.VMEM((3, 3 * c, 3 * c), bf16),
            pltpu.SemaphoreType.DMA((2,)),
        ],
        compiler_params=limit(8),
        name="weights",
    )(
        *far(taps(weight_in), taps(weight_mid)),
        row(gain_in), row(gain_mid), row(bias_in), row(bias_mid), m2,
    )
    keep, send = pl.pallas_call(
        main_body,
        in_specs=[VM] * 11,
        out_specs=(VM,) * 2,
        out_shape=(pltpu.VMEM((2, 2, 2) + tile, f32),) * 2,
        scratch_shapes=[
            pltpu.VMEM((6, 6) + tile, bf16),
            pltpu.VMEM((4, 6) + tile, bf16),
            pltpu.VMEM((6, 4) + tile, bf16),
            pltpu.VMEM((6, 4) + tile, bf16),
            pltpu.VMEM(tile, f32),
            pltpu.VMEM(tile, f32),
            pltpu.VMEM(tile, f32),
            pltpu.VMEM(tile, f32),
        ],
        compiler_params=limit(16),
        name="block",
    )(*near(m1, m2, oc, sp, z1, z2, w1, w2, w1f, w2f, vec))

    got = lax.ppermute(send, "ta", [(0, 1), (1, 0)])
    decoded, grad = pl.pallas_call(
        assemble_body,
        in_specs=[VM] * 2,
        out_shape=(
            jax.ShapeDtypeStruct((n * c * height, width), bf16),
            jax.ShapeDtypeStruct((n * c * height, width), f32),
        ),
        scratch_shapes=[pltpu.VMEM((n * c * height, width), f32)],
        compiler_params=limit(8),
        name="assemble",
    )(*near(keep, got))
    return decoded.reshape(frames.shape), grad.reshape(frames.shape)


def solution(mesh):
    split = P(("grp", "ta"), None, "ha", "wa")
    cache = P("grp", None, "ha", "wa")
    return jax.shard_map(
        per_device,
        mesh=mesh,
        in_specs=(split, cache, cache, P(), P(), P(), P(), P(), P(), split),
        out_specs=(split, split),
        check_vma=False,
    )
```

```python
import jax
import jax.numpy as jnp
from jax import lax
from jax.experimental import pallas as pl
from jax.experimental.pallas import tpu as pltpu
from jax.sharding import PartitionSpec as P


epsilon = 1e-06
f32 = jnp.float32
bf16 = jnp.bfloat16
VM = pl.BlockSpec(memory_space=pltpu.VMEM)
HB = pl.BlockSpec(memory_space=pltpu.HBM)


def near(*values):
    return [pltpu.with_memory_space_constraint(v, pltpu.VMEM) for v in values]


def far(*values):
    return [pltpu.with_memory_space_constraint(v, pltpu.HBM) for v in values]


def lanes_of(shape):
    return lax.broadcasted_iota(jnp.int32, shape, len(shape) - 1)


def act(v, g):
    r = lax.rsqrt(jnp.mean(v * v, axis=0, keepdims=True) + epsilon)
    z = v * r * g
    return z * jax.nn.sigmoid(z)


def act_and_back(v, g, d):
    r = lax.rsqrt(jnp.mean(v * v, axis=0, keepdims=True) + epsilon)
    vr = v * r
    z = vr * g
    s = jax.nn.sigmoid(z)
    q = g * d * s * (1.0 + z * (1.0 - s))
    back = r * q - vr * (r * r) * jnp.mean(q * v, axis=0, keepdims=True)
    return z * s, back


def pack_body(
    fr_far, ct_far, ci_far, cm_far, wi_far, wm_far, gi, gm, bi, bm,
    m1, m2, oc, sw, ed, wi, wm, rows_of, scr, inp, sems,
):
    copies = [
        pltpu.make_async_copy(source, inp.at[i], sems.at[i])
        for i, source in enumerate((fr_far, ct_far, ci_far, cm_far))
    ]
    copies.append(pltpu.make_async_copy(wi_far, wi, sems.at[4]))
    copies.append(pltpu.make_async_copy(wm_far, wm, sems.at[5]))
    for k, source in enumerate((gi, gm, bi, bm)):
        copies.append(pltpu.make_async_copy(source, rows_of.at[k], sems.at[6 + k]))
    for copy in copies:
        copy.start()
    channels = m1.shape[1]
    rows = 4
    flat = channels * rows
    ta = lax.axis_index("ta")
    starts = [(0, 0), (0, flat), (1, 0), (1, flat), (2, ta * flat), (3, ta * flat)]
    starts += [(2, (1 - ta) * flat), (3, (1 - ta) * flat)]
    k = lax.broadcasted_iota(jnp.int32, (rows * 128, 128), 0)
    j = lanes_of((rows * 128, 128))
    column = jnp.where(j % 4 == 0, 1, jnp.where(j % 4 == 1, 0, jnp.where(j % 4 == 2, 127, 126)))
    chosen = (j < 4 * rows) & (k // 128 == j // 4) & (k % 128 == column)
    chosen = jnp.where(chosen, 1.0, 0.0).astype(bf16)
    edges = jnp.zeros((channels, 128), f32)
    for s, (array, start) in enumerate(starts):
        if s in (0, 2, 4, 5):
            copies[array].wait()
        scr[s] = inp[array, pl.ds(start, flat), :].astype(f32)
    for s in range(6):
        tiles = [scr[s, pl.ds(r, channels, stride=rows), :].astype(bf16) for r in range(rows)]
        part = jnp.dot(jnp.concatenate(tiles, axis=1), chosen, preferred_element_type=f32)
        edges = edges + (pltpu.roll(part, 4 * rows * s, 1) if s else part)

        @pl.when(ta == 0)
        def _():
            for i in range(2):
                m1[2 * s + i] = tiles[2 + i]
                m2[2 * s + i] = tiles[i]
                if s < 4:
                    sw[2 * s + i] = tiles[2 + i]
                    sw[8 + 2 * s + i] = tiles[i]

        @pl.when(ta == 1)
        def _():
            for i in range(2):
                m1[2 * s + i] = tiles[i]
                m2[2 * s + i] = tiles[2 + i]
                if s < 4:
                    sw[2 * s + i] = tiles[i]
                    sw[8 + 2 * s + i] = tiles[2 + i]

    for s in range(2):
        for r in range(rows):
            oc[s, r] = scr[6 + s, pl.ds(r, channels, stride=rows), :].astype(bf16)
    ed[...] = edges.astype(bf16)
    for copy in copies[4:]:
        copy.wait()


def merge_body(first, second, sw_in, sw, edge_out):
    even = lax.rem(lax.axis_index("wa"), 2) == 0
    a, b = first[...].astype(f32), second[...].astype(f32)
    inner = lanes_of(a.shape) % 4 >= 2
    edge = jnp.where(inner == even, b, a).astype(bf16)
    edge_out[...] = edge
    sw[16] = edge


def weights_body(win, wmid, rows, after, w1, w2, w1f, w2f, vec):
    channels = w1.shape[0] // 3
    for src, plain, turned in zip((win, wmid), (w1, w2), (w1f, w2f)):
        plain[...] = jnp.concatenate([src[a].astype(f32) for a in range(3)], axis=1).astype(bf16)
        for b in range(3):
            flat = [
                jnp.transpose(src[2 - a, (2 - b) * channels : (3 - b) * channels, :].astype(f32))
                for a in range(3)
            ]
            blocks = [
                flat[a][(2 - t) * channels : (3 - t) * channels] for t in range(3) for a in range(3)
            ]
            turned[b * channels : (b + 1) * channels, :] = jnp.concatenate(blocks, axis=1).astype(
                bf16
            )
    for k in range(4):
        vec[k] = jnp.transpose(jnp.broadcast_to(rows[k], (128, channels)))


def main_body(
    m1, m2, oc, sp, z1, z2, edge, e1, e2, w1, w2, w1f, w2f, vec, keep, send,
    A, C, M, D, PA, PC, EA, EC,
):
    channels = m1.shape[1]
    tile = (channels, 128)
    ta = lax.axis_index("ta")
    ha = lax.axis_index("ha")
    wa = lax.axis_index("wa")
    first_row = (ta == 1) | (ha > 0)
    last_row = (ta == 0) | (ha < lax.axis_size("ha") - 1)
    left_col = wa > 0
    right_col = wa < lax.axis_size("wa") - 1
    other = 1 - ta
    zb = 4 * ta
    mb = 4 - 4 * ta
    lane = lanes_of(tile)
    column = lane % 4
    gin, gmid, bin_, bmid = (vec[k] for k in range(4))

    for i in range(2):
        for r in range(2):
            for src, at, frame, row in (
                (m2, 2 * i + r, 2 * ta + i, 2 + r),
                (m1, 2 * i + r, 2 * ta + i, mb + r),
                (z1, 2 * i + r, 2 * ta + i, zb + r),
                (sp, 2 * i + r, 2 * other + i, 2 + r),
                (sp, 8 + 2 * i + r, 2 * other + i, mb + r),
                (z2, 2 * i + r, 2 * other + i, zb + r),
            ):
                A[2 + frame, row] = act(src[at].astype(f32), gin).astype(bf16)
                C[frame, row] = src[at + 4]
    for r in range(2):
        A[ta, 2 + r] = m2[8 + r]
        A[ta, mb + r] = m1[8 + r]
        A[ta, zb + r] = z1[8 + r]
        A[other, zb + r] = z2[8 + r]
        M[ta, 1 + r] = m2[10 + r]
    M[ta, 3 - 3 * ta] = m1[10 + ta]
    M[ta, 3 * ta] = z1[11 - ta]
    M[other, 3 * ta] = z2[11 - ta]
    for r in range(4):
        A[other, r + 2 - 2 * ta] = oc[0, r]
    for k in range(3):
        M[other, k + 1 - ta] = oc[1, k + ta]

    for e in range(4):
        D[4, e] = jnp.zeros(tile, bf16)
        D[5, e] = jnp.zeros(tile, bf16)

    own, par, zo, zp = (t[...].astype(f32) for t in (edge, sp.at[16], e1, e2))

    def placed(t, slot, start, rows_from, rows, to):
        moved = pltpu.roll(t, (start + 4 * to - 16 * slot - 4 * rows_from) % 128, 1)
        low = start + 4 * to
        return jnp.where((lane >= low) & (lane < low + 4 * rows), moved, 0.0)

    def group(first):
        mine = yours = 0.0
        for i in range(2):
            mine += placed(own, first + i, 32 * i, 0, 4, 2 - 2 * ta)
            mine += placed(zo, first + i, 32 * i, 2 - 2 * ta, 2, 4 * ta)
            yours += placed(par, first + i, 32 * i, 0, 4, 2 - 2 * ta)
            yours += placed(zp, first + i, 32 * i, 2 - 2 * ta, 2, 4 * ta)
        g0 = jnp.where(ta == 0, mine, yours)
        g1 = jnp.where(ta == 0, yours, mine)
        return g0 + pltpu.roll(g1, 64, 1)

    def caches(slot):
        out = placed(own, slot, 32 * ta, 0, 4, 2 - 2 * ta)
        out += placed(zo, slot, 32 * ta, 2 - 2 * ta, 2, 4 * ta)
        out += placed(par, slot, 32 * other, 0, 4, 2 - 2 * ta)
        return out + placed(zp, slot, 32 * other, 2 - 2 * ta, 2, 4 * ta)

    time_first = [(t, a) for t in range(3) for a in range(3)]
    row_first = [(t, a) for a in range(3) for t in range(3)]

    def edge_products(w, low, high, order):
        pieces = []
        for t, a in order:
            s = 32 * t + 4 * a
            if s == 0:
                pieces.append(low.astype(bf16))
                continue
            moved = pltpu.roll(low, 128 - s, 1)
            beyond = 0.0 if high is None else pltpu.roll(high, 128 - s, 1)
            pieces.append(jnp.where(lane < 128 - s, moved, beyond).astype(bf16))
        p = jnp.dot(w[...], jnp.concatenate(pieces, axis=0), preferred_element_type=f32)
        p0, p1, p2 = (p[b * channels : (b + 1) * channels] for b in range(3))
        across = jnp.where(column == 2, p0, p2)
        own_part = jnp.where(column == 2, pltpu.roll(p0, 127, 1), pltpu.roll(p2, 1, 1)) + p1
        return across, own_part

    act_edges = pltpu.roll(act(group(0), gin), 64, 1)
    cin_edges = caches(4)
    across, own_part = edge_products(
        w1, jnp.where(lane < 64, cin_edges, act_edges), jnp.where(lane < 64, act_edges, 0.0),
        row_first,
    )
    PA[...] = across
    EA[...] = own_part
    across, own_part = edge_products(w2f, group(2), None, time_first)
    PC[...] = across
    EC[...] = own_part
    cmid_edges = pltpu.roll(caches(5), 124, 1)

    def products(w, ref, f, row, order):
        cols = [
            jnp.concatenate([ref[f + t, row + i + a] for t, a in order], axis=0) for i in range(2)
        ]
        weights = w[:, : len(order) * channels]
        p = jnp.dot(weights, jnp.concatenate(cols, axis=1), preferred_element_type=f32)
        return [
            [p[b * channels : (b + 1) * channels, 128 * i : 128 * (i + 1)] for b in range(3)]
            for i in range(2)
        ]

    def shifted_sum(p, edge_ref, q):
        back = pltpu.roll(edge_ref[...], lax.rem(256 - (q + 2), 128) if not isinstance(q, int) else (126 - q) % 128, 1)
        out = p[1] + jnp.where(lane == 0, back, pltpu.roll(p[0], 1, 1))
        return out + jnp.where(lane == 127, back, pltpu.roll(p[2], 127, 1))

    def to_edges(p, edge_ref, q):
        moved = pltpu.roll(jnp.where(lane == 0, p[2], p[0]), q + 2, 1)
        here = (lane == q + 1) | (lane == q + 2)
        edge_ref[...] = edge_ref[...] + jnp.where(here, moved, 0.0)

    def first_layer(f):
        for pair in range(2):
            pf = products(w1, A, f, 2 * pair, row_first)
            pb = products(w2f, C, f, 2 * pair, time_first[: 3 * (4 - f)])
            for i in range(2):
                e = 2 * pair + i
                q = f * 32 + e * 4
                hidden = (shifted_sum(pf[i], PA, q) + bin_).astype(bf16).astype(f32)
                back = shifted_sum(pb[i], PC, q)
                to_edges(pf[i], EA, q)
                to_edges(pb[i], EC, q)
                a, d = act_and_back(hidden, gmid, back)
                if e == 0:
                    a = jnp.where(first_row, a, 0.0)
                    d = jnp.where(first_row, d, 0.0)
                if e == 3:
                    a = jnp.where(last_row, a, 0.0)
                    d = jnp.where(last_row, d, 0.0)
                M[2 + f, e] = a.astype(bf16)
                D[f, e] = d.astype(bf16)

    for f in range(4):
        first_layer(f)

    hidden = (EA[...] + bin_).astype(bf16).astype(f32)
    a, d = act_and_back(hidden, gmid, EC[...])
    row = (lane % 32) // 4
    inside = ((column == 2) & left_col) | ((column == 1) & right_col)
    inside = inside & (row < 4) & ((row > 0) | first_row) & ((row < 3) | last_row)
    a = jnp.where(inside, a, 0.0).astype(bf16).astype(f32)
    d = jnp.where(inside, d, 0.0).astype(bf16).astype(f32)
    a = pltpu.roll(a, 64, 1)
    low = jnp.where(lane < 64, cmid_edges, a)
    across, _ = edge_products(w2, low, jnp.where(lane < 64, a, 0.0), row_first)
    PA[...] = across
    across, _ = edge_products(w1f, d, None, time_first)
    PC[...] = across

    def second_layer(f, mine, slot, out):
        pf = products(w2, M, f, 0, row_first)
        pb = products(w1f, D, f, 0, time_first)
        for i in range(2):
            q = f * 32 + i * 4
            frame = mine[2 * slot + i].astype(f32)
            cot = mine[4 + 2 * slot + i].astype(f32)
            decoded = frame + (shifted_sum(pf[i], PA, q) + bmid)
            out[0, slot, i] = decoded.astype(bf16).astype(f32)
            _, back = act_and_back(frame, gin, shifted_sum(pb[i], PC, q))
            out[1, slot, i] = cot + back

    for slot in range(2):
        second_layer(2 * other + slot, sp, slot, send)
    for slot in range(2):
        second_layer(2 * ta + slot, m2, slot, keep)


def assemble_body(keep, got, dec, grad, scr):
    channels = got.shape[3]
    flat = 4 * channels
    ta = lax.axis_index("ta")

    def write(at_keep, at_got):
        for f in range(2):
            for i in range(2):
                for src, r in ((keep, at_keep + i), (got, at_got + i)):
                    scr[pl.ds(f * flat + r, channels, stride=4), :] = src[0, f, i]
                    grad[pl.ds(f * flat + r, channels, stride=4), :] = src[1, f, i]

    @pl.when(ta == 0)
    def _():
        write(0, 2)

    @pl.when(ta == 1)
    def _():
        write(2, 0)

    dec[...] = scr[...].astype(bf16)


def per_device(
    frames, cache_in, cache_mid, gain_in, gain_mid,
    weight_in, bias_in, weight_mid, bias_mid, cotangent,
):
    n, c, height, width = frames.shape
    flat = lambda v: v.reshape(n * c * height, width)
    tile = (c, width)
    limit = lambda mib: pltpu.CompilerParams(vmem_limit_bytes=mib << 20)
    row = lambda v: v.reshape(1, c)
    taps = lambda w: w.reshape(3, 3 * c, 3 * c)
    m1, m2, oc, sw, ed, wi, wm, rows = pl.pallas_call(
        pack_body,
        in_specs=[HB] * 10,
        out_specs=(VM,) * 8,
        out_shape=(
            pltpu.VMEM((12,) + tile, bf16),
            pltpu.VMEM((12,) + tile, bf16),
            pltpu.VMEM((2, 4) + tile, bf16),
            pltpu.VMEM((17,) + tile, bf16),
            pltpu.VMEM(tile, bf16),
            pltpu.VMEM((3, 3 * c, 3 * c), bf16),
            pltpu.VMEM((3, 3 * c, 3 * c), bf16),
            pltpu.VMEM((4, 1, c), f32),
        ),
        scratch_shapes=[
            pltpu.VMEM((8, c * height, width), f32),
            pltpu.VMEM((4, n * c * height, width), bf16),
            pltpu.SemaphoreType.DMA((10,)),
        ],
        compiler_params=limit(8),
        name="pack",
    )(
        *far(
            flat(frames), flat(cotangent), flat(cache_in), flat(cache_mid),
            taps(weight_in), taps(weight_mid),
            row(gain_in), row(gain_mid), row(bias_in), row(bias_mid),
        )
    )

    wide = lax.axis_size("wa")
    high = lax.axis_size("ha")
    pairs = lambda start: [
        p for i in range(start, wide - 1, 2) for p in ((i, i + 1), (i + 1, i))
    ]
    one = [(2 * i, 2 * i + 2) for i in range(high - 1)]
    one += [(2 * i + 3, 2 * i + 1) for i in range(high - 1)]
    two = [(2 * i + 2, 2 * i + 1) for i in range(high - 1)]
    two += [(2 * i + 1, 2 * i + 2) for i in range(high - 1)]
    second = lax.ppermute(ed, "wa", pairs(1))
    first = lax.ppermute(ed, "wa", pairs(0))
    z1 = lax.ppermute(m1, ("ha", "ta"), one)
    z2 = lax.ppermute(m2, ("ha", "ta"), two)
    sw, edge = pl.pallas_call(
        merge_body,
        in_specs=[VM] * 3,
        out_specs=(VM,) * 2,
        out_shape=(pltpu.VMEM((17,) + tile, bf16), pltpu.VMEM(tile, bf16)),
        input_output_aliases={2: 0},
        compiler_params=limit(2),
        name="merge",
    )(*near(first, second, sw))
    sp = lax.ppermute(sw, "ta", [(0, 1), (1, 0)])
    e1 = lax.ppermute(edge, ("ha", "ta"), one)
    e2 = lax.ppermute(edge, ("ha", "ta"), two)

    matrix = pltpu.VMEM((3 * c, 9 * c), bf16)
    w1, w2, w1f, w2f, vec = pl.pallas_call(
        weights_body,
        in_specs=[VM] * 3 + [pl.BlockSpec(memory_space=pl.ANY)],
        out_specs=(VM,) * 5,
        out_shape=(matrix,) * 4 + (pltpu.VMEM((4,) + tile, f32),),
        compiler_params=limit(8),
        name="weights",
    )(*near(wi, wm, rows), edge)
    keep, send = pl.pallas_call(
        main_body,
        in_specs=[VM] * 14,
        out_specs=(VM,) * 2,
        out_shape=(pltpu.VMEM((2, 2, 2) + tile, f32),) * 2,
        scratch_shapes=[
            pltpu.VMEM((6, 6) + tile, bf16),
            pltpu.VMEM((4, 6) + tile, bf16),
            pltpu.VMEM((6, 4) + tile, bf16),
            pltpu.VMEM((6, 4) + tile, bf16),
            pltpu.VMEM(tile, f32),
            pltpu.VMEM(tile, f32),
            pltpu.VMEM(tile, f32),
            pltpu.VMEM(tile, f32),
        ],
        compiler_params=limit(16),
        name="block",
    )(*near(m1, m2, oc, sp, z1, z2, edge, e1, e2, w1, w2, w1f, w2f, vec))

    got = lax.ppermute(send, "ta", [(0, 1), (1, 0)])
    decoded, grad = pl.pallas_call(
        assemble_body,
        in_specs=[VM] * 2,
        out_shape=(
            jax.ShapeDtypeStruct((n * c * height, width), bf16),
            jax.ShapeDtypeStruct((n * c * height, width), f32),
        ),
        scratch_shapes=[pltpu.VMEM((n * c * height, width), f32)],
        compiler_params=limit(8),
        name="assemble",
    )(*near(keep, got))
    return decoded.reshape(frames.shape), grad.reshape(frames.shape)


def solution(mesh):
    split = P(("grp", "ta"), None, "ha", "wa")
    cache = P("grp", None, "ha", "wa")
    return jax.shard_map(
        per_device,
        mesh=mesh,
        in_specs=(split, cache, cache, P(), P(), P(), P(), P(), P(), split),
        out_specs=(split, split),
        check_vma=False,
    )
```

```python
import jax
import jax.numpy as jnp
from jax import lax
from jax.experimental import pallas as pl
from jax.experimental.pallas import tpu as pltpu
from jax.sharding import PartitionSpec as P


epsilon = 1e-06
f32 = jnp.float32
bf16 = jnp.bfloat16
VM = pl.BlockSpec(memory_space=pltpu.VMEM)
HB = pl.BlockSpec(memory_space=pltpu.HBM)


def near(*values):
    return [pltpu.with_memory_space_constraint(v, pltpu.VMEM) for v in values]


def far(*values):
    return [pltpu.with_memory_space_constraint(v, pltpu.HBM) for v in values]


def lanes_of(shape):
    return lax.broadcasted_iota(jnp.int32, shape, len(shape) - 1)


def act(v, g):
    r = lax.rsqrt(jnp.mean(v * v, axis=0, keepdims=True) + epsilon)
    z = v * r * g
    return z * jax.nn.sigmoid(z)


def act_and_back(v, g, d):
    r = lax.rsqrt(jnp.mean(v * v, axis=0, keepdims=True) + epsilon)
    vr = v * r
    z = vr * g
    s = jax.nn.sigmoid(z)
    q = g * d * s * (1.0 + z * (1.0 - s))
    back = r * q - vr * (r * r) * jnp.mean(q * v, axis=0, keepdims=True)
    return z * s, back


def pack_body(
    fr_far, ct_far, ci_far, cm_far, wi_far, wm_far, gi, gm, bi, bm,
    m1, m2, oc, sw, ed, wi, wm, rows_of, scr, inp, sems,
):
    copies = [
        pltpu.make_async_copy(source, inp.at[i], sems.at[i])
        for i, source in enumerate((fr_far, ct_far, ci_far, cm_far))
    ]
    copies.append(pltpu.make_async_copy(wi_far, wi, sems.at[4]))
    copies.append(pltpu.make_async_copy(wm_far, wm, sems.at[5]))
    for k, source in enumerate((gi, gm, bi, bm)):
        copies.append(pltpu.make_async_copy(source, rows_of.at[k], sems.at[6 + k]))
    for copy in copies:
        copy.start()
    channels = m1.shape[1]
    rows = 4
    flat = channels * rows
    ta = lax.axis_index("ta")
    starts = [(0, 0), (0, flat), (1, 0), (1, flat), (2, ta * flat), (3, ta * flat)]
    starts += [(2, (1 - ta) * flat), (3, (1 - ta) * flat)]
    k = lax.broadcasted_iota(jnp.int32, (rows * 128, 128), 0)
    j = lanes_of((rows * 128, 128))
    column = jnp.where(j % 4 == 0, 1, jnp.where(j % 4 == 1, 0, jnp.where(j % 4 == 2, 127, 126)))
    chosen = (j < 4 * rows) & (k // 128 == j // 4) & (k % 128 == column)
    chosen = jnp.where(chosen, 1.0, 0.0).astype(bf16)
    edges = jnp.zeros((channels, 128), f32)
    for s, (array, start) in enumerate(starts):
        if s in (0, 2, 4, 5):
            copies[array].wait()
        scr[s] = inp[array, pl.ds(start, flat), :].astype(f32)
    for s in range(6):
        tiles = [scr[s, pl.ds(r, channels, stride=rows), :].astype(bf16) for r in range(rows)]
        part = jnp.dot(jnp.concatenate(tiles, axis=1), chosen, preferred_element_type=f32)
        edges = edges + (pltpu.roll(part, 4 * rows * s, 1) if s else part)

        @pl.when(ta == 0)
        def _():
            for i in range(2):
                m1[2 * s + i] = tiles[2 + i]
                m2[2 * s + i] = tiles[i]
                if s < 4:
                    sw[2 * s + i] = tiles[2 + i]
                    sw[8 + 2 * s + i] = tiles[i]

        @pl.when(ta == 1)
        def _():
            for i in range(2):
                m1[2 * s + i] = tiles[i]
                m2[2 * s + i] = tiles[2 + i]
                if s < 4:
                    sw[2 * s + i] = tiles[i]
                    sw[8 + 2 * s + i] = tiles[2 + i]

    for s in range(2):
        for r in range(rows):
            oc[s, r] = scr[6 + s, pl.ds(r, channels, stride=rows), :].astype(bf16)
    ed[...] = edges.astype(bf16)
    for copy in copies[4:]:
        copy.wait()


def merge_body(first, second, sw_in, sw, edge_out):
    even = lax.rem(lax.axis_index("wa"), 2) == 0
    a, b = first[...].astype(f32), second[...].astype(f32)
    inner = lanes_of(a.shape) % 4 >= 2
    edge = jnp.where(inner == even, b, a).astype(bf16)
    edge_out[...] = edge
    sw[16] = edge


def weights_body(win, wmid, rows, after, w1, w2, w1f, w2f, vec):
    channels = w1.shape[0] // 3
    for src, plain, turned in zip((win, wmid), (w1, w2), (w1f, w2f)):
        plain[...] = jnp.concatenate([src[a].astype(f32) for a in range(3)], axis=1).astype(bf16)
        for b in range(3):
            flat = [
                jnp.transpose(src[2 - a, (2 - b) * channels : (3 - b) * channels, :].astype(f32))
                for a in range(3)
            ]
            blocks = [
                flat[a][(2 - t) * channels : (3 - t) * channels] for t in range(3) for a in range(3)
            ]
            turned[b * channels : (b + 1) * channels, :] = jnp.concatenate(blocks, axis=1).astype(
                bf16
            )
    for k in range(4):
        vec[k] = jnp.transpose(jnp.broadcast_to(rows[k], (128, channels)))


def offsets():
    ta = lax.axis_index("ta")
    return ta, 1 - ta, 4 * ta, 4 - 4 * ta


time_first = [(t, a) for t in range(3) for a in range(3)]
row_first = [(t, a) for a in range(3) for t in range(3)]


def lead_body(m1, m2, oc, vec, after, A, C, M):
    ta, other, _, mb = offsets()
    gin = vec[0]
    for i in range(2):
        for r in range(2):
            for src, row in ((m2, 2 + r), (m1, mb + r)):
                at = 2 * i + r
                A[2 + 2 * ta + i, row] = act(src[at].astype(f32), gin).astype(bf16)
                C[2 * ta + i, row] = src[at + 4]
    for r in range(2):
        A[ta, 2 + r] = m2[8 + r]
        A[ta, mb + r] = m1[8 + r]
        M[ta, 1 + r] = m2[10 + r]
    M[ta, 3 - 3 * ta] = m1[10 + ta]
    for r in range(4):
        A[other, r + 2 - 2 * ta] = oc[0, r]
    for k in range(3):
        M[other, k + 1 - ta] = oc[1, k + ta]


def products(w, ref, f, row, order):
    channels = ref.shape[2]
    cols = [jnp.concatenate([ref[f + t, row + i + a] for t, a in order], axis=0) for i in range(2)]
    weights = w[:, : len(order) * channels]
    p = jnp.dot(weights, jnp.concatenate(cols, axis=1), preferred_element_type=f32)
    return [
        [p[b * channels : (b + 1) * channels, 128 * i : 128 * (i + 1)] for b in range(3)]
        for i in range(2)
    ]


def shifted_sum(p, edge_ref, q):
    lane = lanes_of(p[1].shape)
    amount = (126 - q) % 128 if isinstance(q, int) else lax.rem(254 - q, 128)
    back = pltpu.roll(edge_ref[...], amount, 1)
    out = p[1] + jnp.where(lane == 0, back, pltpu.roll(p[0], 1, 1))
    return out + jnp.where(lane == 127, back, pltpu.roll(p[2], 127, 1))


def second_layer(f, mine, slot, out, M, D, PA, PC, w2, w1f, vec):
    pf = products(w2, M, f, 0, row_first)
    pb = products(w1f, D, f, 0, time_first)
    for i in range(2):
        q = f * 32 + i * 4
        frame = mine[2 * slot + i].astype(f32)
        cot = mine[4 + 2 * slot + i].astype(f32)
        decoded = frame + (shifted_sum(pf[i], PA, q) + vec[3])
        out[0, slot, i] = decoded.astype(bf16).astype(f32)
        _, back = act_and_back(frame, vec[0], shifted_sum(pb[i], PC, q))
        out[1, slot, i] = cot + back


def own_body(m2, M, D, PA, PC, w2, w1f, vec, keep):
    ta = lax.axis_index("ta")
    for slot in range(2):
        second_layer(2 * ta + slot, m2, slot, keep, M, D, PA, PC, w2, w1f, vec)


def main_body(
    A_in, C_in, M_in, sp, z1, z2, edge, e1, e2, w1, w2, w1f, w2f, vec,
    A, C, M, D, PA, PC, send, EA, EC,
):
    channels = sp.shape[1]
    tile = (channels, 128)
    ta, other, zb, mb = offsets()
    ha = lax.axis_index("ha")
    wa = lax.axis_index("wa")
    first_row = (ta == 1) | (ha > 0)
    last_row = (ta == 0) | (ha < lax.axis_size("ha") - 1)
    left_col = wa > 0
    right_col = wa < lax.axis_size("wa") - 1
    lane = lanes_of(tile)
    column = lane % 4
    gin, gmid, bin_, _ = (vec[k] for k in range(4))

    for i in range(2):
        for r in range(2):
            for src, at, frame, row in (
                (z1, 2 * i + r, 2 * ta + i, zb + r),
                (sp, 2 * i + r, 2 * other + i, 2 + r),
                (sp, 8 + 2 * i + r, 2 * other + i, mb + r),
                (z2, 2 * i + r, 2 * other + i, zb + r),
            ):
                A[2 + frame, row] = act(src[at].astype(f32), gin).astype(bf16)
                C[frame, row] = src[at + 4]
    for r in range(2):
        A[ta, zb + r] = z1[8 + r]
        A[other, zb + r] = z2[8 + r]
    M[ta, 3 * ta] = z1[11 - ta]
    M[other, 3 * ta] = z2[11 - ta]
    for e in range(4):
        D[4, e] = jnp.zeros(tile, bf16)
        D[5, e] = jnp.zeros(tile, bf16)

    own, par, zo, zp = (t[...].astype(f32) for t in (edge, sp.at[16], e1, e2))

    def placed(t, slot, start, rows_from, rows, to):
        moved = pltpu.roll(t, (start + 4 * to - 16 * slot - 4 * rows_from) % 128, 1)
        low = start + 4 * to
        return jnp.where((lane >= low) & (lane < low + 4 * rows), moved, 0.0)

    def group(first):
        mine = yours = 0.0
        for i in range(2):
            mine += placed(own, first + i, 32 * i, 0, 4, 2 - 2 * ta)
            mine += placed(zo, first + i, 32 * i, 2 - 2 * ta, 2, 4 * ta)
            yours += placed(par, first + i, 32 * i, 0, 4, 2 - 2 * ta)
            yours += placed(zp, first + i, 32 * i, 2 - 2 * ta, 2, 4 * ta)
        g0 = jnp.where(ta == 0, mine, yours)
        g1 = jnp.where(ta == 0, yours, mine)
        return g0 + pltpu.roll(g1, 64, 1)

    def caches(slot):
        out = placed(own, slot, 32 * ta, 0, 4, 2 - 2 * ta)
        out += placed(zo, slot, 32 * ta, 2 - 2 * ta, 2, 4 * ta)
        out += placed(par, slot, 32 * other, 0, 4, 2 - 2 * ta)
        return out + placed(zp, slot, 32 * other, 2 - 2 * ta, 2, 4 * ta)

    def edge_products(w, low, high, order):
        pieces = []
        for t, a in order:
            s = 32 * t + 4 * a
            if s == 0:
                pieces.append(low.astype(bf16))
                continue
            moved = pltpu.roll(low, 128 - s, 1)
            beyond = 0.0 if high is None else pltpu.roll(high, 128 - s, 1)
            pieces.append(jnp.where(lane < 128 - s, moved, beyond).astype(bf16))
        p = jnp.dot(w[...], jnp.concatenate(pieces, axis=0), preferred_element_type=f32)
        p0, p1, p2 = (p[b * channels : (b + 1) * channels] for b in range(3))
        across = jnp.where(column == 2, p0, p2)
        own_part = jnp.where(column == 2, pltpu.roll(p0, 127, 1), pltpu.roll(p2, 1, 1)) + p1
        return across, own_part

    act_edges = pltpu.roll(act(group(0), gin), 64, 1)
    cin_edges = caches(4)
    across, own_part = edge_products(
        w1, jnp.where(lane < 64, cin_edges, act_edges), jnp.where(lane < 64, act_edges, 0.0),
        row_first,
    )
    PA[...] = across
    EA[...] = own_part
    across, own_part = edge_products(w2f, group(2), None, time_first)
    PC[...] = across
    EC[...] = own_part
    cmid_edges = pltpu.roll(caches(5), 124, 1)

    def to_edges(p, edge_ref, q):
        moved = pltpu.roll(jnp.where(lane == 0, p[2], p[0]), q + 2, 1)
        here = (lane == q + 1) | (lane == q + 2)
        edge_ref[...] = edge_ref[...] + jnp.where(here, moved, 0.0)

    def first_layer(f):
        for pair in range(2):
            pf = products(w1, A, f, 2 * pair, row_first)
            pb = products(w2f, C, f, 2 * pair, time_first[: 3 * (4 - f)])
            for i in range(2):
                e = 2 * pair + i
                q = f * 32 + e * 4
                hidden = (shifted_sum(pf[i], PA, q) + bin_).astype(bf16).astype(f32)
                back = shifted_sum(pb[i], PC, q)
                to_edges(pf[i], EA, q)
                to_edges(pb[i], EC, q)
                a, d = act_and_back(hidden, gmid, back)
                if e == 0:
                    a = jnp.where(first_row, a, 0.0)
                    d = jnp.where(first_row, d, 0.0)
                if e == 3:
                    a = jnp.where(last_row, a, 0.0)
                    d = jnp.where(last_row, d, 0.0)
                M[2 + f, e] = a.astype(bf16)
                D[f, e] = d.astype(bf16)

    for f in range(4):
        first_layer(f)

    hidden = (EA[...] + bin_).astype(bf16).astype(f32)
    a, d = act_and_back(hidden, gmid, EC[...])
    row = (lane % 32) // 4
    inside = ((column == 2) & left_col) | ((column == 1) & right_col)
    inside = inside & (row < 4) & ((row > 0) | first_row) & ((row < 3) | last_row)
    a = jnp.where(inside, a, 0.0).astype(bf16).astype(f32)
    d = jnp.where(inside, d, 0.0).astype(bf16).astype(f32)
    a = pltpu.roll(a, 64, 1)
    low = jnp.where(lane < 64, cmid_edges, a)
    across, _ = edge_products(w2, low, jnp.where(lane < 64, a, 0.0), row_first)
    PA[...] = across
    across, _ = edge_products(w1f, d, None, time_first)
    PC[...] = across

    for slot in range(2):
        second_layer(2 * other + slot, sp, slot, send, M, D, PA, PC, w2, w1f, vec)


def assemble_body(keep, got, dec, grad, scr):
    channels = got.shape[3]
    flat = 4 * channels
    ta = lax.axis_index("ta")

    def write(at_keep, at_got):
        for f in range(2):
            for i in range(2):
                for src, r in ((keep, at_keep + i), (got, at_got + i)):
                    scr[pl.ds(f * flat + r, channels, stride=4), :] = src[0, f, i]
                    grad[pl.ds(f * flat + r, channels, stride=4), :] = src[1, f, i]

    @pl.when(ta == 0)
    def _():
        write(0, 2)

    @pl.when(ta == 1)
    def _():
        write(2, 0)

    dec[...] = scr[...].astype(bf16)


def per_device(
    frames, cache_in, cache_mid, gain_in, gain_mid,
    weight_in, bias_in, weight_mid, bias_mid, cotangent,
):
    n, c, height, width = frames.shape
    flat = lambda v: v.reshape(n * c * height, width)
    tile = (c, width)
    limit = lambda mib: pltpu.CompilerParams(vmem_limit_bytes=mib << 20)
    row = lambda v: v.reshape(1, c)
    taps = lambda w: w.reshape(3, 3 * c, 3 * c)
    m1, m2, oc, sw, ed, wi, wm, rows = pl.pallas_call(
        pack_body,
        in_specs=[HB] * 10,
        out_specs=(VM,) * 8,
        out_shape=(
            pltpu.VMEM((12,) + tile, bf16),
            pltpu.VMEM((12,) + tile, bf16),
            pltpu.VMEM((2, 4) + tile, bf16),
            pltpu.VMEM((17,) + tile, bf16),
            pltpu.VMEM(tile, bf16),
            pltpu.VMEM((3, 3 * c, 3 * c), bf16),
            pltpu.VMEM((3, 3 * c, 3 * c), bf16),
            pltpu.VMEM((4, 1, c), f32),
        ),
        scratch_shapes=[
            pltpu.VMEM((8, c * height, width), f32),
            pltpu.VMEM((4, n * c * height, width), bf16),
            pltpu.SemaphoreType.DMA((10,)),
        ],
        compiler_params=limit(8),
        name="pack",
    )(
        *far(
            flat(frames), flat(cotangent), flat(cache_in), flat(cache_mid),
            taps(weight_in), taps(weight_mid),
            row(gain_in), row(gain_mid), row(bias_in), row(bias_mid),
        )
    )

    wide = lax.axis_size("wa")
    high = lax.axis_size("ha")
    pairs = lambda start: [
        p for i in range(start, wide - 1, 2) for p in ((i, i + 1), (i + 1, i))
    ]
    one = [(2 * i, 2 * i + 2) for i in range(high - 1)]
    one += [(2 * i + 3, 2 * i + 1) for i in range(high - 1)]
    two = [(2 * i + 2, 2 * i + 1) for i in range(high - 1)]
    two += [(2 * i + 1, 2 * i + 2) for i in range(high - 1)]
    second = lax.ppermute(ed, "wa", pairs(1))
    first = lax.ppermute(ed, "wa", pairs(0))
    z1 = lax.ppermute(m1, ("ha", "ta"), one)
    z2 = lax.ppermute(m2, ("ha", "ta"), two)
    sw, edge = pl.pallas_call(
        merge_body,
        in_specs=[VM] * 3,
        out_specs=(VM,) * 2,
        out_shape=(pltpu.VMEM((17,) + tile, bf16), pltpu.VMEM(tile, bf16)),
        input_output_aliases={2: 0},
        compiler_params=limit(2),
        name="merge",
    )(*near(first, second, sw))
    sp = lax.ppermute(sw, "ta", [(0, 1), (1, 0)])
    e1 = lax.ppermute(edge, ("ha", "ta"), one)
    e2 = lax.ppermute(edge, ("ha", "ta"), two)

    matrix = pltpu.VMEM((3 * c, 9 * c), bf16)
    w1, w2, w1f, w2f, vec = pl.pallas_call(
        weights_body,
        in_specs=[VM] * 3 + [pl.BlockSpec(memory_space=pl.ANY)],
        out_specs=(VM,) * 5,
        out_shape=(matrix,) * 4 + (pltpu.VMEM((4,) + tile, f32),),
        compiler_params=limit(8),
        name="weights",
    )(*near(wi, wm, rows), m2)
    staged = (
        pltpu.VMEM((6, 6) + tile, bf16),
        pltpu.VMEM((4, 6) + tile, bf16),
        pltpu.VMEM((6, 4) + tile, bf16),
    )
    A, C, M = pl.pallas_call(
        lead_body,
        in_specs=[VM] * 4 + [pl.BlockSpec(memory_space=pl.ANY)],
        out_specs=(VM,) * 3,
        out_shape=staged,
        compiler_params=limit(8),
        name="lead",
    )(*near(m1, m2, oc, vec), edge)
    half = pltpu.VMEM((2, 2, 2) + tile, f32)
    A, C, M, D, PA, PC, send = pl.pallas_call(
        main_body,
        in_specs=[VM] * 14,
        out_specs=(VM,) * 7,
        out_shape=staged
        + (
            pltpu.VMEM((6, 4) + tile, bf16),
            pltpu.VMEM(tile, f32),
            pltpu.VMEM(tile, f32),
            half,
        ),
        scratch_shapes=[pltpu.VMEM(tile, f32), pltpu.VMEM(tile, f32)],
        input_output_aliases={0: 0, 1: 1, 2: 2},
        compiler_params=limit(12),
        name="block",
    )(*near(A, C, M, sp, z1, z2, edge, e1, e2, w1, w2, w1f, w2f, vec))
    got = lax.ppermute(send, "ta", [(0, 1), (1, 0)])
    keep = pl.pallas_call(
        own_body,
        in_specs=[VM] * 8,
        out_specs=VM,
        out_shape=half,
        compiler_params=limit(8),
        name="own",
    )(*near(m2, M, D, PA, PC, w2, w1f, vec))
    decoded, grad = pl.pallas_call(
        assemble_body,
        in_specs=[VM] * 2,
        out_shape=(
            jax.ShapeDtypeStruct((n * c * height, width), bf16),
            jax.ShapeDtypeStruct((n * c * height, width), f32),
        ),
        scratch_shapes=[pltpu.VMEM((n * c * height, width), f32)],
        compiler_params=limit(8),
        name="assemble",
    )(*near(keep, got))
    return decoded.reshape(frames.shape), grad.reshape(frames.shape)


def solution(mesh):
    split = P(("grp", "ta"), None, "ha", "wa")
    cache = P("grp", None, "ha", "wa")
    return jax.shard_map(
        per_device,
        mesh=mesh,
        in_specs=(split, cache, cache, P(), P(), P(), P(), P(), P(), split),
        out_specs=(split, split),
        check_vma=False,
    )
```

```python
import jax
import jax.numpy as jnp
from jax import lax
from jax.experimental import pallas as pl
from jax.experimental.pallas import tpu as pltpu
from jax.sharding import PartitionSpec as P


epsilon = 1e-06
f32 = jnp.float32
bf16 = jnp.bfloat16
VM = pl.BlockSpec(memory_space=pltpu.VMEM)
HB = pl.BlockSpec(memory_space=pltpu.HBM)


def near(*values):
    return [pltpu.with_memory_space_constraint(v, pltpu.VMEM) for v in values]


def far(*values):
    return [pltpu.with_memory_space_constraint(v, pltpu.HBM) for v in values]


def lanes_of(shape):
    return lax.broadcasted_iota(jnp.int32, shape, len(shape) - 1)


def act(v, g):
    r = lax.rsqrt(jnp.mean(v * v, axis=0, keepdims=True) + epsilon)
    z = v * r * g
    return z * jax.nn.sigmoid(z)


def act_and_back(v, g, d):
    r = lax.rsqrt(jnp.mean(v * v, axis=0, keepdims=True) + epsilon)
    vr = v * r
    z = vr * g
    s = jax.nn.sigmoid(z)
    q = g * d * s * (1.0 + z * (1.0 - s))
    back = r * q - vr * (r * r) * jnp.mean(q * v, axis=0, keepdims=True)
    return z * s, back


def pack_body(
    fr_far, ct_far, ci_far, cm_far, wi_far, wm_far, gi, gm, bi, bm,
    m1, m2, oc, sw, ed, wi, wm, rows_of, scr, inp, sems,
):
    copies = [
        pltpu.make_async_copy(source, inp.at[i], sems.at[i])
        for i, source in enumerate((fr_far, ct_far, ci_far, cm_far))
    ]
    copies.append(pltpu.make_async_copy(wi_far, wi, sems.at[4]))
    copies.append(pltpu.make_async_copy(wm_far, wm, sems.at[5]))
    for k, source in enumerate((gi, gm, bi, bm)):
        copies.append(pltpu.make_async_copy(source, rows_of.at[k], sems.at[6 + k]))
    for copy in copies:
        copy.start()
    channels = m1.shape[1]
    rows = 4
    flat = channels * rows
    ta = lax.axis_index("ta")
    starts = [(0, 0), (0, flat), (1, 0), (1, flat), (2, ta * flat), (3, ta * flat)]
    starts += [(2, (1 - ta) * flat), (3, (1 - ta) * flat)]
    k = lax.broadcasted_iota(jnp.int32, (rows * 128, 128), 0)
    j = lanes_of((rows * 128, 128))
    column = jnp.where(j % 4 == 0, 1, jnp.where(j % 4 == 1, 0, jnp.where(j % 4 == 2, 127, 126)))
    chosen = (j < 4 * rows) & (k // 128 == j // 4) & (k % 128 == column)
    chosen = jnp.where(chosen, 1.0, 0.0).astype(bf16)
    edges = jnp.zeros((channels, 128), f32)
    for s, (array, start) in enumerate(starts):
        if s in (0, 2, 4, 5):
            copies[array].wait()
        scr[s] = inp[array, pl.ds(start, flat), :].astype(f32)
    for s in range(6):
        tiles = [scr[s, pl.ds(r, channels, stride=rows), :].astype(bf16) for r in range(rows)]
        part = jnp.dot(jnp.concatenate(tiles, axis=1), chosen, preferred_element_type=f32)
        edges = edges + (pltpu.roll(part, 4 * rows * s, 1) if s else part)

        @pl.when(ta == 0)
        def _():
            for i in range(2):
                m1[2 * s + i] = tiles[2 + i]
                m2[2 * s + i] = tiles[i]
                if s < 4:
                    sw[2 * s + i] = tiles[2 + i]
                    sw[8 + 2 * s + i] = tiles[i]

        @pl.when(ta == 1)
        def _():
            for i in range(2):
                m1[2 * s + i] = tiles[i]
                m2[2 * s + i] = tiles[2 + i]
                if s < 4:
                    sw[2 * s + i] = tiles[i]
                    sw[8 + 2 * s + i] = tiles[2 + i]

    for s in range(2):
        for r in range(rows):
            oc[s, r] = scr[6 + s, pl.ds(r, channels, stride=rows), :].astype(bf16)
    ed[...] = edges.astype(bf16)
    for copy in copies[4:]:
        copy.wait()


def merge_body(first, second, sw_in, sw, edge_out):
    even = lax.rem(lax.axis_index("wa"), 2) == 0
    a, b = first[...].astype(f32), second[...].astype(f32)
    inner = lanes_of(a.shape) % 4 >= 2
    edge = jnp.where(inner == even, b, a).astype(bf16)
    edge_out[...] = edge
    sw[16] = edge


def weights_body(win, wmid, rows, after, w1, w2, w1f, w2f, vec):
    channels = w1.shape[0] // 3
    for src, plain, turned in zip((win, wmid), (w1, w2), (w1f, w2f)):
        plain[...] = jnp.concatenate([src[a].astype(f32) for a in range(3)], axis=1).astype(bf16)
        for b in range(3):
            flat = [
                jnp.transpose(src[2 - a, (2 - b) * channels : (3 - b) * channels, :].astype(f32))
                for a in range(3)
            ]
            blocks = [
                flat[a][(2 - t) * channels : (3 - t) * channels] for t in range(3) for a in range(3)
            ]
            turned[b * channels : (b + 1) * channels, :] = jnp.concatenate(blocks, axis=1).astype(
                bf16
            )
    for k in range(4):
        vec[k] = jnp.transpose(jnp.broadcast_to(rows[k], (128, channels)))


def offsets():
    ta = lax.axis_index("ta")
    return ta, 1 - ta, 4 * ta, 4 - 4 * ta


time_first = [(t, a) for t in range(3) for a in range(3)]
row_first = [(t, a) for a in range(3) for t in range(3)]


def lead_body(m1, m2, oc, z1, z2, vec, A, C, M):
    ta, other, zb, mb = offsets()
    gin = vec[0]
    for i in range(2):
        for r in range(2):
            at = 2 * i + r
            for src, frame, row in (
                (m2, 2 * ta + i, 2 + r),
                (m1, 2 * ta + i, mb + r),
                (z1, 2 * ta + i, zb + r),
                (z2, 2 * other + i, zb + r),
            ):
                A[2 + frame, row] = act(src[at].astype(f32), gin).astype(bf16)
                C[frame, row] = src[at + 4]
    for r in range(2):
        A[ta, 2 + r] = m2[8 + r]
        A[ta, mb + r] = m1[8 + r]
        A[ta, zb + r] = z1[8 + r]
        A[other, zb + r] = z2[8 + r]
        M[ta, 1 + r] = m2[10 + r]
    M[ta, 3 - 3 * ta] = m1[10 + ta]
    M[ta, 3 * ta] = z1[11 - ta]
    M[other, 3 * ta] = z2[11 - ta]
    for r in range(4):
        A[other, r + 2 - 2 * ta] = oc[0, r]
    for k in range(3):
        M[other, k + 1 - ta] = oc[1, k + ta]


def products(w, ref, f, row, order):
    channels = ref.shape[2]
    cols = [jnp.concatenate([ref[f + t, row + i + a] for t, a in order], axis=0) for i in range(2)]
    weights = w[:, : len(order) * channels]
    p = jnp.dot(weights, jnp.concatenate(cols, axis=1), preferred_element_type=f32)
    return [
        [p[b * channels : (b + 1) * channels, 128 * i : 128 * (i + 1)] for b in range(3)]
        for i in range(2)
    ]


def shifted_sum(p, edge_ref, q):
    lane = lanes_of(p[1].shape)
    amount = (126 - q) % 128 if isinstance(q, int) else lax.rem(254 - q, 128)
    back = pltpu.roll(edge_ref[...], amount, 1)
    out = p[1] + jnp.where(lane == 0, back, pltpu.roll(p[0], 1, 1))
    return out + jnp.where(lane == 127, back, pltpu.roll(p[2], 127, 1))


def second_products(f, M, D, w2, w1f):
    return products(w2, M, f, 0, row_first), products(w1f, D, f, 0, time_first)


def second_layer(f, mine, slot, out, both, PA, PC, vec):
    pf, pb = both
    for i in range(2):
        q = f * 32 + i * 4
        frame = mine[2 * slot + i].astype(f32)
        cot = mine[4 + 2 * slot + i].astype(f32)
        decoded = frame + (shifted_sum(pf[i], PA, q) + vec[3])
        out[0, slot, i] = decoded.astype(bf16).astype(f32)
        _, back = act_and_back(frame, vec[0], shifted_sum(pb[i], PC, q))
        out[1, slot, i] = cot + back


def own_body(m2, M, D, PA, PC, w2, w1f, vec, keep):
    ta = lax.axis_index("ta")
    for slot in range(2):
        f = 2 * ta + slot
        second_layer(f, m2, slot, keep, second_products(f, M, D, w2, w1f), PA, PC, vec)


def main_body(
    A_in, C_in, M_in, sp, edge, e1, e2, w1, w2, w1f, w2f, vec,
    A, C, M, D, PA, PC, send, EA, EC,
):
    channels = sp.shape[1]
    tile = (channels, 128)
    ta, other, _, mb = offsets()
    ha = lax.axis_index("ha")
    wa = lax.axis_index("wa")
    first_row = (ta == 1) | (ha > 0)
    last_row = (ta == 0) | (ha < lax.axis_size("ha") - 1)
    left_col = wa > 0
    right_col = wa < lax.axis_size("wa") - 1
    lane = lanes_of(tile)
    column = lane % 4
    gin, gmid, bin_, _ = (vec[k] for k in range(4))

    for i in range(2):
        for r in range(2):
            for src, at, frame, row in (
                (sp, 2 * i + r, 2 * other + i, 2 + r),
                (sp, 8 + 2 * i + r, 2 * other + i, mb + r),
            ):
                A[2 + frame, row] = act(src[at].astype(f32), gin).astype(bf16)
                C[frame, row] = src[at + 4]
    for e in range(4):
        D[4, e] = jnp.zeros(tile, bf16)
        D[5, e] = jnp.zeros(tile, bf16)

    own, par, zo, zp = (t[...].astype(f32) for t in (edge, sp.at[16], e1, e2))

    def placed(t, slot, start, rows_from, rows, to):
        moved = pltpu.roll(t, (start + 4 * to - 16 * slot - 4 * rows_from) % 128, 1)
        low = start + 4 * to
        return jnp.where((lane >= low) & (lane < low + 4 * rows), moved, 0.0)

    def group(first):
        mine = yours = 0.0
        for i in range(2):
            mine += placed(own, first + i, 32 * i, 0, 4, 2 - 2 * ta)
            mine += placed(zo, first + i, 32 * i, 2 - 2 * ta, 2, 4 * ta)
            yours += placed(par, first + i, 32 * i, 0, 4, 2 - 2 * ta)
            yours += placed(zp, first + i, 32 * i, 2 - 2 * ta, 2, 4 * ta)
        g0 = jnp.where(ta == 0, mine, yours)
        g1 = jnp.where(ta == 0, yours, mine)
        return g0 + pltpu.roll(g1, 64, 1)

    def caches(slot):
        out = placed(own, slot, 32 * ta, 0, 4, 2 - 2 * ta)
        out += placed(zo, slot, 32 * ta, 2 - 2 * ta, 2, 4 * ta)
        out += placed(par, slot, 32 * other, 0, 4, 2 - 2 * ta)
        return out + placed(zp, slot, 32 * other, 2 - 2 * ta, 2, 4 * ta)

    def edge_products(w, low, high, order, last=False):
        pieces = []
        for t, a in order:
            s = 32 * t + 4 * a
            if s == 0:
                pieces.append(low.astype(bf16))
                continue
            moved = pltpu.roll(low, 128 - s, 1)
            beyond = 0.0 if high is None else pltpu.roll(high, 128 - s, 1)
            pieces.append(jnp.where(lane < 128 - s, moved, beyond).astype(bf16))
        stacked = jnp.concatenate(pieces, axis=0)
        if last:
            outer = jnp.concatenate([w[:channels, :], w[2 * channels :, :]], axis=0)
            p = jnp.dot(outer, stacked, preferred_element_type=f32)
            return jnp.where(column == 2, p[:channels], p[channels:])
        p = jnp.dot(w[...], stacked, preferred_element_type=f32)
        p0, p1, p2 = (p[b * channels : (b + 1) * channels] for b in range(3))
        across = jnp.where(column == 2, p0, p2)
        own_part = jnp.where(column == 2, pltpu.roll(p0, 127, 1), pltpu.roll(p2, 1, 1)) + p1
        return across, own_part

    def to_edges(p, edge_ref, q):
        moved = pltpu.roll(jnp.where(lane == 0, p[2], p[0]), q + 2, 1)
        here = (lane == q + 1) | (lane == q + 2)
        edge_ref[...] = edge_ref[...] + jnp.where(here, moved, 0.0)

    def first_products(f, pair):
        pf = products(w1, A, f, 2 * pair, row_first)
        return pf, products(w2f, C, f, 2 * pair, time_first[: 3 * (4 - f)])

    early = [first_products(0, pair) for pair in range(2)]
    act_edges = pltpu.roll(act(group(0), gin), 64, 1)
    cin_edges = caches(4)
    across, own_part = edge_products(
        w1, jnp.where(lane < 64, cin_edges, act_edges), jnp.where(lane < 64, act_edges, 0.0),
        row_first,
    )
    PA[...] = across
    EA[...] = own_part
    across, own_part = edge_products(w2f, group(2), None, time_first)
    PC[...] = across
    EC[...] = own_part
    cmid_edges = pltpu.roll(caches(5), 124, 1)

    def first_layer(f):
        for pair in range(2):
            pf, pb = early[pair] if f == 0 else first_products(f, pair)
            for i in range(2):
                e = 2 * pair + i
                q = f * 32 + e * 4
                hidden = (shifted_sum(pf[i], PA, q) + bin_).astype(bf16).astype(f32)
                back = shifted_sum(pb[i], PC, q)
                to_edges(pf[i], EA, q)
                to_edges(pb[i], EC, q)
                a, d = act_and_back(hidden, gmid, back)
                if e == 0:
                    a = jnp.where(first_row, a, 0.0)
                    d = jnp.where(first_row, d, 0.0)
                if e == 3:
                    a = jnp.where(last_row, a, 0.0)
                    d = jnp.where(last_row, d, 0.0)
                M[2 + f, e] = a.astype(bf16)
                D[f, e] = d.astype(bf16)

    for f in range(4):
        first_layer(f)

    late = [second_products(2 * other + slot, M, D, w2, w1f) for slot in range(2)]
    hidden = (EA[...] + bin_).astype(bf16).astype(f32)
    a, d = act_and_back(hidden, gmid, EC[...])
    row = (lane % 32) // 4
    inside = ((column == 2) & left_col) | ((column == 1) & right_col)
    inside = inside & (row < 4) & ((row > 0) | first_row) & ((row < 3) | last_row)
    a = jnp.where(inside, a, 0.0).astype(bf16).astype(f32)
    d = jnp.where(inside, d, 0.0).astype(bf16).astype(f32)
    a = pltpu.roll(a, 64, 1)
    low = jnp.where(lane < 64, cmid_edges, a)
    PA[...] = edge_products(w2, low, jnp.where(lane < 64, a, 0.0), row_first, last=True)
    PC[...] = edge_products(w1f, d, None, time_first, last=True)

    for slot in range(2):
        second_layer(2 * other + slot, sp, slot, send, late[slot], PA, PC, vec)


def assemble_body(keep, got, dec, grad, scr):
    channels = got.shape[3]
    flat = 4 * channels
    ta = lax.axis_index("ta")

    def write(at_keep, at_got):
        for f in range(2):
            for i in range(2):
                for src, r in ((keep, at_keep + i), (got, at_got + i)):
                    scr[pl.ds(f * flat + r, channels, stride=4), :] = src[0, f, i]
                    grad[pl.ds(f * flat + r, channels, stride=4), :] = src[1, f, i]

    @pl.when(ta == 0)
    def _():
        write(0, 2)

    @pl.when(ta == 1)
    def _():
        write(2, 0)

    dec[...] = scr[...].astype(bf16)


def per_device(
    frames, cache_in, cache_mid, gain_in, gain_mid,
    weight_in, bias_in, weight_mid, bias_mid, cotangent,
):
    n, c, height, width = frames.shape
    flat = lambda v: v.reshape(n * c * height, width)
    tile = (c, width)
    limit = lambda mib: pltpu.CompilerParams(vmem_limit_bytes=mib << 20)
    row = lambda v: v.reshape(1, c)
    taps = lambda w: w.reshape(3, 3 * c, 3 * c)
    m1, m2, oc, sw, ed, wi, wm, rows = pl.pallas_call(
        pack_body,
        in_specs=[HB] * 10,
        out_specs=(VM,) * 8,
        out_shape=(
            pltpu.VMEM((12,) + tile, bf16),
            pltpu.VMEM((12,) + tile, bf16),
            pltpu.VMEM((2, 4) + tile, bf16),
            pltpu.VMEM((17,) + tile, bf16),
            pltpu.VMEM(tile, bf16),
            pltpu.VMEM((3, 3 * c, 3 * c), bf16),
            pltpu.VMEM((3, 3 * c, 3 * c), bf16),
            pltpu.VMEM((4, 1, c), f32),
        ),
        scratch_shapes=[
            pltpu.VMEM((8, c * height, width), f32),
            pltpu.VMEM((4, n * c * height, width), bf16),
            pltpu.SemaphoreType.DMA((10,)),
        ],
        compiler_params=limit(8),
        name="pack",
    )(
        *far(
            flat(frames), flat(cotangent), flat(cache_in), flat(cache_mid),
            taps(weight_in), taps(weight_mid),
            row(gain_in), row(gain_mid), row(bias_in), row(bias_mid),
        )
    )

    wide = lax.axis_size("wa")
    high = lax.axis_size("ha")
    pairs = lambda start: [
        p for i in range(start, wide - 1, 2) for p in ((i, i + 1), (i + 1, i))
    ]
    one = [(2 * i, 2 * i + 2) for i in range(high - 1)]
    one += [(2 * i + 3, 2 * i + 1) for i in range(high - 1)]
    two = [(2 * i + 2, 2 * i + 1) for i in range(high - 1)]
    two += [(2 * i + 1, 2 * i + 2) for i in range(high - 1)]
    second = lax.ppermute(ed, "wa", pairs(1))
    first = lax.ppermute(ed, "wa", pairs(0))
    z1 = lax.ppermute(m1, ("ha", "ta"), one)
    z2 = lax.ppermute(m2, ("ha", "ta"), two)
    sw, edge = pl.pallas_call(
        merge_body,
        in_specs=[VM] * 3,
        out_specs=(VM,) * 2,
        out_shape=(pltpu.VMEM((17,) + tile, bf16), pltpu.VMEM(tile, bf16)),
        input_output_aliases={2: 0},
        compiler_params=limit(2),
        name="merge",
    )(*near(first, second, sw))
    sp = lax.ppermute(sw, "ta", [(0, 1), (1, 0)])
    e1 = lax.ppermute(edge, ("ha", "ta"), one)
    e2 = lax.ppermute(edge, ("ha", "ta"), two)

    matrix = pltpu.VMEM((3 * c, 9 * c), bf16)
    w1, w2, w1f, w2f, vec = pl.pallas_call(
        weights_body,
        in_specs=[VM] * 3 + [pl.BlockSpec(memory_space=pl.ANY)],
        out_specs=(VM,) * 5,
        out_shape=(matrix,) * 4 + (pltpu.VMEM((4,) + tile, f32),),
        compiler_params=limit(8),
        name="weights",
    )(*near(wi, wm, rows), m2)
    staged = (
        pltpu.VMEM((6, 6) + tile, bf16),
        pltpu.VMEM((4, 6) + tile, bf16),
        pltpu.VMEM((6, 4) + tile, bf16),
    )
    A, C, M = pl.pallas_call(
        lead_body,
        in_specs=[VM] * 6,
        out_specs=(VM,) * 3,
        out_shape=staged,
        compiler_params=limit(8),
        name="lead",
    )(*near(m1, m2, oc, z1, z2, vec))
    half = pltpu.VMEM((2, 2, 2) + tile, f32)
    A, C, M, D, PA, PC, send = pl.pallas_call(
        main_body,
        in_specs=[VM] * 12,
        out_specs=(VM,) * 7,
        out_shape=staged
        + (
            pltpu.VMEM((6, 4) + tile, bf16),
            pltpu.VMEM(tile, f32),
            pltpu.VMEM(tile, f32),
            half,
        ),
        scratch_shapes=[pltpu.VMEM(tile, f32), pltpu.VMEM(tile, f32)],
        input_output_aliases={0: 0, 1: 1, 2: 2},
        compiler_params=limit(12),
        name="block",
    )(*near(A, C, M, sp, edge, e1, e2, w1, w2, w1f, w2f, vec))
    got = lax.ppermute(send, "ta", [(0, 1), (1, 0)])
    keep = pl.pallas_call(
        own_body,
        in_specs=[VM] * 8,
        out_specs=VM,
        out_shape=half,
        compiler_params=limit(8),
        name="own",
    )(*near(m2, M, D, PA, PC, w2, w1f, vec))
    decoded, grad = pl.pallas_call(
        assemble_body,
        in_specs=[VM] * 2,
        out_shape=(
            jax.ShapeDtypeStruct((n * c * height, width), bf16),
            jax.ShapeDtypeStruct((n * c * height, width), f32),
        ),
        scratch_shapes=[pltpu.VMEM((n * c * height, width), f32)],
        compiler_params=limit(8),
        name="assemble",
    )(*near(keep, got))
    return decoded.reshape(frames.shape), grad.reshape(frames.shape)


def solution(mesh):
    split = P(("grp", "ta"), None, "ha", "wa")
    cache = P("grp", None, "ha", "wa")
    return jax.shard_map(
        per_device,
        mesh=mesh,
        in_specs=(split, cache, cache, P(), P(), P(), P(), P(), P(), split),
        out_specs=(split, split),
        check_vma=False,
    )
```

```python
import jax
import jax.numpy as jnp
from jax import lax
from jax.experimental import pallas as pl
from jax.experimental.pallas import tpu as pltpu
from jax.sharding import PartitionSpec as P


epsilon = 1e-06
f32 = jnp.float32
bf16 = jnp.bfloat16
VM = pl.BlockSpec(memory_space=pltpu.VMEM)
HB = pl.BlockSpec(memory_space=pltpu.HBM)


def near(*values):
    return [pltpu.with_memory_space_constraint(v, pltpu.VMEM) for v in values]


def far(*values):
    return [pltpu.with_memory_space_constraint(v, pltpu.HBM) for v in values]


def lanes_of(shape):
    return lax.broadcasted_iota(jnp.int32, shape, len(shape) - 1)


def act(v, g):
    r = lax.rsqrt(jnp.mean(v * v, axis=0, keepdims=True) + epsilon)
    z = v * r * g
    return z * jax.nn.sigmoid(z)


def act_and_back(v, g, d):
    r = lax.rsqrt(jnp.mean(v * v, axis=0, keepdims=True) + epsilon)
    vr = v * r
    z = vr * g
    s = jax.nn.sigmoid(z)
    q = g * d * s * (1.0 + z * (1.0 - s))
    back = r * q - vr * (r * r) * jnp.mean(q * v, axis=0, keepdims=True)
    return z * s, back


def fetch_body(
    fr_far, ct_far, ci_far, cm_far, wi_far, wm_far, gi, gm, bi, bm,
    ed, scr, wi, wm, rows_of, inp, sems, others,
):
    channels = ed.shape[0]
    rows = 4
    flat = channels * rows
    quarter = inp.shape[1] // 4
    copies = [
        [
            pltpu.make_async_copy(
                source.at[pl.ds(k * quarter, quarter)],
                inp.at[i, pl.ds(k * quarter, quarter)],
                sems.at[4 * i + k],
            )
            for k in range(4)
        ]
        for i, source in enumerate((fr_far, ct_far, ci_far, cm_far))
    ]
    rest = [pltpu.make_async_copy(wi_far, wi, others.at[0])]
    rest.append(pltpu.make_async_copy(wm_far, wm, others.at[1]))
    for k, source in enumerate((gi, gm, bi, bm)):
        rest.append(pltpu.make_async_copy(source, rows_of.at[k], others.at[2 + k]))
    for group in copies + [rest]:
        for copy in group:
            copy.start()
    ta = lax.axis_index("ta")
    starts = [(0, 0), (0, flat), (1, 0), (1, flat), (2, ta * flat), (3, ta * flat)]
    starts += [(2, (1 - ta) * flat), (3, (1 - ta) * flat)]
    k = lax.broadcasted_iota(jnp.int32, (rows * 128, 128), 0)
    j = lanes_of((rows * 128, 128))
    column = jnp.where(j % 4 == 0, 1, jnp.where(j % 4 == 1, 0, jnp.where(j % 4 == 2, 127, 126)))
    chosen = (j < 4 * rows) & (k // 128 == j // 4) & (k % 128 == column)
    chosen = jnp.where(chosen, 1.0, 0.0).astype(bf16)
    edges = jnp.zeros((channels, 128), f32)
    for s, (array, start) in enumerate(starts):
        if s in (0, 2, 4, 5):
            for copy in copies[array]:
                copy.wait()
        scr[s] = inp[array, pl.ds(start, flat), :].astype(f32)
    for s in range(6):
        tiles = [scr[s, pl.ds(r, channels, stride=rows), :].astype(bf16) for r in range(rows)]
        part = jnp.dot(jnp.concatenate(tiles, axis=1), chosen, preferred_element_type=f32)
        edges = edges + (pltpu.roll(part, 4 * rows * s, 1) if s else part)
    ed[...] = edges.astype(bf16)
    for copy in rest:
        copy.wait()


def pack_body(scr, m1, m2, oc, sw):
    channels = m1.shape[1]
    ta = lax.axis_index("ta")
    tile_of = lambda s, r: scr[s, pl.ds(r, channels, stride=4), :].astype(bf16)
    for s in range(6):
        for i in range(2):
            far_half = tile_of(s, 2 - 2 * ta + i)
            own_half = tile_of(s, 2 * ta + i)
            m1[2 * s + i] = far_half
            m2[2 * s + i] = own_half
            if s < 4:
                sw[2 * s + i] = far_half
                sw[8 + 2 * s + i] = own_half
    for s in range(2):
        for r in range(4):
            oc[s, r] = tile_of(6 + s, r)


def merge_body(first, second, sw_in, sw, edge_out):
    even = lax.rem(lax.axis_index("wa"), 2) == 0
    a, b = first[...].astype(f32), second[...].astype(f32)
    inner = lanes_of(a.shape) % 4 >= 2
    edge = jnp.where(inner == even, b, a).astype(bf16)
    edge_out[...] = edge
    sw[16] = edge


def weights_body(win, wmid, rows, after, w1, w2, w1f, w2f, vec):
    channels = w1.shape[0] // 3
    for src, plain, turned in zip((win, wmid), (w1, w2), (w1f, w2f)):
        plain[...] = jnp.concatenate([src[a].astype(f32) for a in range(3)], axis=1).astype(bf16)
        for b in range(3):
            flat = [
                jnp.transpose(src[2 - a, (2 - b) * channels : (3 - b) * channels, :].astype(f32))
                for a in range(3)
            ]
            blocks = [
                flat[a][(2 - t) * channels : (3 - t) * channels] for t in range(3) for a in range(3)
            ]
            turned[b * channels : (b + 1) * channels, :] = jnp.concatenate(blocks, axis=1).astype(
                bf16
            )
    for k in range(4):
        vec[k] = jnp.transpose(jnp.broadcast_to(rows[k], (128, channels)))


def offsets():
    ta = lax.axis_index("ta")
    return ta, 1 - ta, 4 * ta, 4 - 4 * ta


time_first = [(t, a) for t in range(3) for a in range(3)]
row_first = [(t, a) for a in range(3) for t in range(3)]


def lead_body(m1, m2, oc, z1, z2, vec, A, C, M):
    ta, other, zb, mb = offsets()
    gin = vec[0]
    for i in range(2):
        for r in range(2):
            at = 2 * i + r
            for src, frame, row in (
                (m2, 2 * ta + i, 2 + r),
                (m1, 2 * ta + i, mb + r),
                (z1, 2 * ta + i, zb + r),
                (z2, 2 * other + i, zb + r),
            ):
                A[2 + frame, row] = act(src[at].astype(f32), gin).astype(bf16)
                C[frame, row] = src[at + 4]
    for r in range(2):
        A[ta, 2 + r] = m2[8 + r]
        A[ta, mb + r] = m1[8 + r]
        A[ta, zb + r] = z1[8 + r]
        A[other, zb + r] = z2[8 + r]
        M[ta, 1 + r] = m2[10 + r]
    M[ta, 3 - 3 * ta] = m1[10 + ta]
    M[ta, 3 * ta] = z1[11 - ta]
    M[other, 3 * ta] = z2[11 - ta]
    for r in range(4):
        A[other, r + 2 - 2 * ta] = oc[0, r]
    for k in range(3):
        M[other, k + 1 - ta] = oc[1, k + ta]


def products(w, ref, f, row, order):
    channels = ref.shape[2]
    cols = [jnp.concatenate([ref[f + t, row + i + a] for t, a in order], axis=0) for i in range(2)]
    weights = w[:, : len(order) * channels]
    p = jnp.dot(weights, jnp.concatenate(cols, axis=1), preferred_element_type=f32)
    return [
        [p[b * channels : (b + 1) * channels, 128 * i : 128 * (i + 1)] for b in range(3)]
        for i in range(2)
    ]


def shifted_sum(p, edge_ref, q):
    lane = lanes_of(p[1].shape)
    amount = (126 - q) % 128 if isinstance(q, int) else lax.rem(254 - q, 128)
    back = pltpu.roll(edge_ref[...], amount, 1)
    out = p[1] + jnp.where(lane == 0, back, pltpu.roll(p[0], 1, 1))
    return out + jnp.where(lane == 127, back, pltpu.roll(p[2], 127, 1))


def second_products(f, M, D, w2, w1f):
    return products(w2, M, f, 0, row_first), products(w1f, D, f, 0, time_first)


def second_layer(f, mine, slot, out, both, PA, PC, vec):
    pf, pb = both
    for i in range(2):
        q = f * 32 + i * 4
        frame = mine[2 * slot + i].astype(f32)
        cot = mine[4 + 2 * slot + i].astype(f32)
        decoded = frame + (shifted_sum(pf[i], PA, q) + vec[3])
        out[0, slot, i] = decoded.astype(bf16).astype(f32)
        _, back = act_and_back(frame, vec[0], shifted_sum(pb[i], PC, q))
        out[1, slot, i] = cot + back


def own_body(m2, M, D, PA, PC, w2, w1f, vec, keep):
    ta = lax.axis_index("ta")
    for slot in range(2):
        f = 2 * ta + slot
        second_layer(f, m2, slot, keep, second_products(f, M, D, w2, w1f), PA, PC, vec)


def main_body(
    A_in, C_in, M_in, sp, edge, e1, e2, w1, w2, w1f, w2f, vec,
    A, C, M, D, PA, PC, send, EA, EC,
):
    channels = sp.shape[1]
    tile = (channels, 128)
    ta, other, _, mb = offsets()
    ha = lax.axis_index("ha")
    wa = lax.axis_index("wa")
    first_row = (ta == 1) | (ha > 0)
    last_row = (ta == 0) | (ha < lax.axis_size("ha") - 1)
    left_col = wa > 0
    right_col = wa < lax.axis_size("wa") - 1
    lane = lanes_of(tile)
    column = lane % 4
    gin, gmid, bin_, _ = (vec[k] for k in range(4))

    for i in range(2):
        for r in range(2):
            for src, at, frame, row in (
                (sp, 2 * i + r, 2 * other + i, 2 + r),
                (sp, 8 + 2 * i + r, 2 * other + i, mb + r),
            ):
                A[2 + frame, row] = act(src[at].astype(f32), gin).astype(bf16)
                C[frame, row] = src[at + 4]
    for e in range(4):
        D[4, e] = jnp.zeros(tile, bf16)
        D[5, e] = jnp.zeros(tile, bf16)

    own, par, zo, zp = (t[...].astype(f32) for t in (edge, sp.at[16], e1, e2))

    def placed(t, slot, start, rows_from, rows, to):
        moved = pltpu.roll(t, (start + 4 * to - 16 * slot - 4 * rows_from) % 128, 1)
        low = start + 4 * to
        return jnp.where((lane >= low) & (lane < low + 4 * rows), moved, 0.0)

    def group(first):
        mine = yours = 0.0
        for i in range(2):
            mine += placed(own, first + i, 32 * i, 0, 4, 2 - 2 * ta)
            mine += placed(zo, first + i, 32 * i, 2 - 2 * ta, 2, 4 * ta)
            yours += placed(par, first + i, 32 * i, 0, 4, 2 - 2 * ta)
            yours += placed(zp, first + i, 32 * i, 2 - 2 * ta, 2, 4 * ta)
        g0 = jnp.where(ta == 0, mine, yours)
        g1 = jnp.where(ta == 0, yours, mine)
        return g0 + pltpu.roll(g1, 64, 1)

    def caches(slot):
        out = placed(own, slot, 32 * ta, 0, 4, 2 - 2 * ta)
        out += placed(zo, slot, 32 * ta, 2 - 2 * ta, 2, 4 * ta)
        out += placed(par, slot, 32 * other, 0, 4, 2 - 2 * ta)
        return out + placed(zp, slot, 32 * other, 2 - 2 * ta, 2, 4 * ta)

    def edge_products(w, low, high, order, last=False):
        pieces = []
        for t, a in order:
            s = 32 * t + 4 * a
            if s == 0:
                pieces.append(low.astype(bf16))
                continue
            moved = pltpu.roll(low, 128 - s, 1)
            beyond = 0.0 if high is None else pltpu.roll(high, 128 - s, 1)
            pieces.append(jnp.where(lane < 128 - s, moved, beyond).astype(bf16))
        stacked = jnp.concatenate(pieces, axis=0)
        if last:
            outer = jnp.concatenate([w[:channels, :], w[2 * channels :, :]], axis=0)
            p = jnp.dot(outer, stacked, preferred_element_type=f32)
            return jnp.where(column == 2, p[:channels], p[channels:])
        p = jnp.dot(w[...], stacked, preferred_element_type=f32)
        p0, p1, p2 = (p[b * channels : (b + 1) * channels] for b in range(3))
        across = jnp.where(column == 2, p0, p2)
        own_part = jnp.where(column == 2, pltpu.roll(p0, 127, 1), pltpu.roll(p2, 1, 1)) + p1
        return across, own_part

    def to_edges(p, edge_ref, q):
        moved = pltpu.roll(jnp.where(lane == 0, p[2], p[0]), q + 2, 1)
        here = (lane == q + 1) | (lane == q + 2)
        edge_ref[...] = edge_ref[...] + jnp.where(here, moved, 0.0)

    def first_products(f, pair):
        pf = products(w1, A, f, 2 * pair, row_first)
        return pf, products(w2f, C, f, 2 * pair, time_first[: 3 * (4 - f)])

    early = [first_products(0, pair) for pair in range(2)]
    act_edges = pltpu.roll(act(group(0), gin), 64, 1)
    cin_edges = caches(4)
    across, own_part = edge_products(
        w1, jnp.where(lane < 64, cin_edges, act_edges), jnp.where(lane < 64, act_edges, 0.0),
        row_first,
    )
    PA[...] = across
    EA[...] = own_part
    across, own_part = edge_products(w2f, group(2), None, time_first)
    PC[...] = across
    EC[...] = own_part
    cmid_edges = pltpu.roll(caches(5), 124, 1)

    def first_layer(f):
        for pair in range(2):
            pf, pb = early[pair] if f == 0 else first_products(f, pair)
            for i in range(2):
                e = 2 * pair + i
                q = f * 32 + e * 4
                hidden = (shifted_sum(pf[i], PA, q) + bin_).astype(bf16).astype(f32)
                back = shifted_sum(pb[i], PC, q)
                to_edges(pf[i], EA, q)
                to_edges(pb[i], EC, q)
                a, d = act_and_back(hidden, gmid, back)
                if e == 0:
                    a = jnp.where(first_row, a, 0.0)
                    d = jnp.where(first_row, d, 0.0)
                if e == 3:
                    a = jnp.where(last_row, a, 0.0)
                    d = jnp.where(last_row, d, 0.0)
                M[2 + f, e] = a.astype(bf16)
                D[f, e] = d.astype(bf16)

    for f in range(4):
        first_layer(f)

    late = [second_products(2 * other + slot, M, D, w2, w1f) for slot in range(2)]
    hidden = (EA[...] + bin_).astype(bf16).astype(f32)
    a, d = act_and_back(hidden, gmid, EC[...])
    row = (lane % 32) // 4
    inside = ((column == 2) & left_col) | ((column == 1) & right_col)
    inside = inside & (row < 4) & ((row > 0) | first_row) & ((row < 3) | last_row)
    a = jnp.where(inside, a, 0.0).astype(bf16).astype(f32)
    d = jnp.where(inside, d, 0.0).astype(bf16).astype(f32)
    a = pltpu.roll(a, 64, 1)
    low = jnp.where(lane < 64, cmid_edges, a)
    PA[...] = edge_products(w2, low, jnp.where(lane < 64, a, 0.0), row_first, last=True)
    PC[...] = edge_products(w1f, d, None, time_first, last=True)

    for slot in range(2):
        second_layer(2 * other + slot, sp, slot, send, late[slot], PA, PC, vec)


def assemble_body(keep, got, dec, grad, scr):
    channels = got.shape[3]
    flat = 4 * channels
    ta = lax.axis_index("ta")

    def write(at_keep, at_got):
        for f in range(2):
            for i in range(2):
                for src, r in ((keep, at_keep + i), (got, at_got + i)):
                    scr[pl.ds(f * flat + r, channels, stride=4), :] = src[0, f, i]
                    grad[pl.ds(f * flat + r, channels, stride=4), :] = src[1, f, i]

    @pl.when(ta == 0)
    def _():
        write(0, 2)

    @pl.when(ta == 1)
    def _():
        write(2, 0)

    dec[...] = scr[...].astype(bf16)


def per_device(
    frames, cache_in, cache_mid, gain_in, gain_mid,
    weight_in, bias_in, weight_mid, bias_mid, cotangent,
):
    n, c, height, width = frames.shape
    flat = lambda v: v.reshape(n * c * height, width)
    tile = (c, width)
    limit = lambda mib: pltpu.CompilerParams(vmem_limit_bytes=mib << 20)
    row = lambda v: v.reshape(1, c)
    taps = lambda w: w.reshape(3, 3 * c, 3 * c)
    ed, scr, wi, wm, rows = pl.pallas_call(
        fetch_body,
        in_specs=[HB] * 10,
        out_specs=(VM,) * 5,
        out_shape=(
            pltpu.VMEM(tile, bf16),
            pltpu.VMEM((8, c * height, width), f32),
            pltpu.VMEM((3, 3 * c, 3 * c), bf16),
            pltpu.VMEM((3, 3 * c, 3 * c), bf16),
            pltpu.VMEM((4, 1, c), f32),
        ),
        scratch_shapes=[
            pltpu.VMEM((4, n * c * height, width), bf16),
            pltpu.SemaphoreType.DMA((16,)),
            pltpu.SemaphoreType.DMA((6,)),
        ],
        compiler_params=limit(6),
        name="fetch",
    )(
        *far(
            flat(frames), flat(cotangent), flat(cache_in), flat(cache_mid),
            taps(weight_in), taps(weight_mid),
            row(gain_in), row(gain_mid), row(bias_in), row(bias_mid),
        )
    )
    m1, m2, oc, sw = pl.pallas_call(
        pack_body,
        in_specs=[VM],
        out_specs=(VM,) * 4,
        out_shape=(
            pltpu.VMEM((12,) + tile, bf16),
            pltpu.VMEM((12,) + tile, bf16),
            pltpu.VMEM((2, 4) + tile, bf16),
            pltpu.VMEM((17,) + tile, bf16),
        ),
        compiler_params=limit(4),
        name="pack",
    )(*near(scr))

    wide = lax.axis_size("wa")
    high = lax.axis_size("ha")
    pairs = lambda start: [
        p for i in range(start, wide - 1, 2) for p in ((i, i + 1), (i + 1, i))
    ]
    one = [(2 * i, 2 * i + 2) for i in range(high - 1)]
    one += [(2 * i + 3, 2 * i + 1) for i in range(high - 1)]
    two = [(2 * i + 2, 2 * i + 1) for i in range(high - 1)]
    two += [(2 * i + 1, 2 * i + 2) for i in range(high - 1)]
    second = lax.ppermute(ed, "wa", pairs(1))
    first = lax.ppermute(ed, "wa", pairs(0))
    z1 = lax.ppermute(m1, ("ha", "ta"), one)
    z2 = lax.ppermute(m2, ("ha", "ta"), two)
    sw, edge = pl.pallas_call(
        merge_body,
        in_specs=[VM] * 3,
        out_specs=(VM,) * 2,
        out_shape=(pltpu.VMEM((17,) + tile, bf16), pltpu.VMEM(tile, bf16)),
        input_output_aliases={2: 0},
        compiler_params=limit(2),
        name="merge",
    )(*near(first, second, sw))
    sp = lax.ppermute(sw, "ta", [(0, 1), (1, 0)])
    e1 = lax.ppermute(edge, ("ha", "ta"), one)
    e2 = lax.ppermute(edge, ("ha", "ta"), two)

    matrix = pltpu.VMEM((3 * c, 9 * c), bf16)
    w1, w2, w1f, w2f, vec = pl.pallas_call(
        weights_body,
        in_specs=[VM] * 3 + [pl.BlockSpec(memory_space=pl.ANY)],
        out_specs=(VM,) * 5,
        out_shape=(matrix,) * 4 + (pltpu.VMEM((4,) + tile, f32),),
        compiler_params=limit(8),
        name="weights",
    )(*near(wi, wm, rows), m2)
    staged = (
        pltpu.VMEM((6, 6) + tile, bf16),
        pltpu.VMEM((4, 6) + tile, bf16),
        pltpu.VMEM((6, 4) + tile, bf16),
    )
    A, C, M = pl.pallas_call(
        lead_body,
        in_specs=[VM] * 6,
        out_specs=(VM,) * 3,
        out_shape=staged,
        compiler_params=limit(8),
        name="lead",
    )(*near(m1, m2, oc, z1, z2, vec))
    half = pltpu.VMEM((2, 2, 2) + tile, f32)
    A, C, M, D, PA, PC, send = pl.pallas_call(
        main_body,
        in_specs=[VM] * 12,
        out_specs=(VM,) * 7,
        out_shape=staged
        + (
            pltpu.VMEM((6, 4) + tile, bf16),
            pltpu.VMEM(tile, f32),
            pltpu.VMEM(tile, f32),
            half,
        ),
        scratch_shapes=[pltpu.VMEM(tile, f32), pltpu.VMEM(tile, f32)],
        input_output_aliases={0: 0, 1: 1, 2: 2},
        compiler_params=limit(12),
        name="block",
    )(*near(A, C, M, sp, edge, e1, e2, w1, w2, w1f, w2f, vec))
    got = lax.ppermute(send, "ta", [(0, 1), (1, 0)])
    keep = pl.pallas_call(
        own_body,
        in_specs=[VM] * 8,
        out_specs=VM,
        out_shape=half,
        compiler_params=limit(8),
        name="own",
    )(*near(m2, M, D, PA, PC, w2, w1f, vec))
    decoded, grad = pl.pallas_call(
        assemble_body,
        in_specs=[VM] * 2,
        out_shape=(
            jax.ShapeDtypeStruct((n * c * height, width), bf16),
            jax.ShapeDtypeStruct((n * c * height, width), f32),
        ),
        scratch_shapes=[pltpu.VMEM((n * c * height, width), f32)],
        compiler_params=limit(8),
        name="assemble",
    )(*near(keep, got))
    return decoded.reshape(frames.shape), grad.reshape(frames.shape)


def solution(mesh):
    split = P(("grp", "ta"), None, "ha", "wa")
    cache = P("grp", None, "ha", "wa")
    return jax.shard_map(
        per_device,
        mesh=mesh,
        in_specs=(split, cache, cache, P(), P(), P(), P(), P(), P(), split),
        out_specs=(split, split),
        check_vma=False,
    )
```

```python
import jax
import jax.numpy as jnp
from jax import lax
from jax.experimental import pallas as pl
from jax.experimental.pallas import tpu as pltpu
from jax.sharding import PartitionSpec as P


epsilon = 1e-06
f32 = jnp.float32
bf16 = jnp.bfloat16
VM = pl.BlockSpec(memory_space=pltpu.VMEM)
HB = pl.BlockSpec(memory_space=pltpu.HBM)


def near(*values):
    return [pltpu.with_memory_space_constraint(v, pltpu.VMEM) for v in values]


def far(*values):
    return [pltpu.with_memory_space_constraint(v, pltpu.HBM) for v in values]


def lanes_of(shape):
    return lax.broadcasted_iota(jnp.int32, shape, len(shape) - 1)


def act(v, g):
    r = lax.rsqrt(jnp.mean(v * v, axis=0, keepdims=True) + epsilon)
    z = v * r * g
    return z * jax.nn.sigmoid(z)


def act_and_back(v, g, d):
    r = lax.rsqrt(jnp.mean(v * v, axis=0, keepdims=True) + epsilon)
    vr = v * r
    z = vr * g
    s = jax.nn.sigmoid(z)
    q = g * d * s * (1.0 + z * (1.0 - s))
    back = r * q - vr * (r * r) * jnp.mean(q * v, axis=0, keepdims=True)
    return z * s, back


def fetch_body(
    fr_far, ct_far, ci_far, cm_far, gi, gm, bi, bm,
    ed, scr, rows_of, inp, sems, others,
):
    channels = ed.shape[0]
    rows = 4
    flat = channels * rows
    quarter = inp.shape[1] // 4
    copies = [
        [
            pltpu.make_async_copy(
                source.at[pl.ds(k * quarter, quarter)],
                inp.at[i, pl.ds(k * quarter, quarter)],
                sems.at[4 * i + k],
            )
            for k in range(4)
        ]
        for i, source in enumerate((fr_far, ct_far, ci_far, cm_far))
    ]
    rest = [
        pltpu.make_async_copy(source, rows_of.at[k], others.at[k])
        for k, source in enumerate((gi, gm, bi, bm))
    ]
    for group in copies + [rest]:
        for copy in group:
            copy.start()
    ta = lax.axis_index("ta")
    starts = [(0, 0), (0, flat), (1, 0), (1, flat), (2, ta * flat), (3, ta * flat)]
    starts += [(2, (1 - ta) * flat), (3, (1 - ta) * flat)]
    k = lax.broadcasted_iota(jnp.int32, (rows * 128, 128), 0)
    j = lanes_of((rows * 128, 128))
    column = jnp.where(j % 4 == 0, 1, jnp.where(j % 4 == 1, 0, jnp.where(j % 4 == 2, 127, 126)))
    chosen = (j < 4 * rows) & (k // 128 == j // 4) & (k % 128 == column)
    chosen = jnp.where(chosen, 1.0, 0.0).astype(bf16)
    edges = jnp.zeros((channels, 128), f32)
    for s, (array, start) in enumerate(starts):
        if s in (0, 2, 4, 5):
            for copy in copies[array]:
                copy.wait()
        scr[s] = inp[array, pl.ds(start, flat), :].astype(f32)
    for s in range(6):
        tiles = [scr[s, pl.ds(r, channels, stride=rows), :].astype(bf16) for r in range(rows)]
        part = jnp.dot(jnp.concatenate(tiles, axis=1), chosen, preferred_element_type=f32)
        edges = edges + (pltpu.roll(part, 4 * rows * s, 1) if s else part)
    ed[...] = edges.astype(bf16)
    for copy in rest:
        copy.wait()


def pack_body(scr, early_weight, m1, m2, oc, sw):
    channels = m1.shape[1]
    ta = lax.axis_index("ta")
    tile_of = lambda s, r: scr[s, pl.ds(r, channels, stride=4), :].astype(bf16)
    for s in range(6):
        for i in range(2):
            far_half = tile_of(s, 2 - 2 * ta + i)
            own_half = tile_of(s, 2 * ta + i)
            m1[2 * s + i] = far_half
            m2[2 * s + i] = own_half
            if s < 4:
                sw[2 * s + i] = far_half
                sw[8 + 2 * s + i] = own_half
    for s in range(2):
        for r in range(4):
            oc[s, r] = tile_of(6 + s, r)


def merge_body(first, second, sw_in, sw, edge_out):
    even = lax.rem(lax.axis_index("wa"), 2) == 0
    a, b = first[...].astype(f32), second[...].astype(f32)
    inner = lanes_of(a.shape) % 4 >= 2
    edge = jnp.where(inner == even, b, a).astype(bf16)
    edge_out[...] = edge
    sw[16] = edge


def weights_body(win, wmid, rows, after, ws, w2, w1f, vec):
    channels = w2.shape[0] // 3
    w1, w2f = ws.at[0], ws.at[1]
    for src, plain, turned in zip((win, wmid), (w1, w2), (w1f, w2f)):
        plain[...] = jnp.concatenate([src[a].astype(f32) for a in range(3)], axis=1).astype(bf16)
        for b in range(3):
            flat = [
                jnp.transpose(src[2 - a, (2 - b) * channels : (3 - b) * channels, :].astype(f32))
                for a in range(3)
            ]
            blocks = [
                flat[a][(2 - t) * channels : (3 - t) * channels] for a in range(3) for t in range(3)
            ]
            turned[b * channels : (b + 1) * channels, :] = jnp.concatenate(blocks, axis=1).astype(
                bf16
            )
    for k in range(4):
        vec[k] = jnp.transpose(jnp.broadcast_to(rows[k], (128, channels)))


def offsets():
    ta = lax.axis_index("ta")
    return ta, 1 - ta, 4 * ta, 4 - 4 * ta


taps_order = [(t, a) for a in range(3) for t in range(3)]


def product(weights, ref, lead, f, row):
    cols = [
        jnp.concatenate([ref[lead + (f + t, row + i + a)] for t, a in taps_order], axis=0)
        for i in range(2)
    ]
    return jnp.dot(weights, jnp.concatenate(cols, axis=1), preferred_element_type=f32)


def parts(p):
    n = p.shape[0] // 3
    return [[p[b * n : (b + 1) * n, 128 * i : 128 * (i + 1)] for b in range(3)] for i in range(2)]


def partial_products(ws, AC, PV, which):
    for k in range(2):
        for pair in range(2):
            PV[which, k, pair] = product(ws[which], AC, (which,), 2 * which + k, 2 * pair)


def lead_body(m1, m2, oc, z1, z2, vec, ws, AC, M, PV):
    A, C = AC.at[0], AC.at[1]
    ta, other, zb, mb = offsets()
    gin = vec[0]
    for i in range(2):
        for r in range(2):
            at = 2 * i + r
            for src, frame, row in (
                (m2, 2 * ta + i, 2 + r),
                (m1, 2 * ta + i, mb + r),
                (z1, 2 * ta + i, zb + r),
                (z2, 2 * other + i, zb + r),
            ):
                A[2 + frame, row] = act(src[at].astype(f32), gin).astype(bf16)
                C[frame, row] = src[at + 4]
    for r in range(2):
        A[ta, 2 + r] = m2[8 + r]
        A[ta, mb + r] = m1[8 + r]
        A[ta, zb + r] = z1[8 + r]
        A[other, zb + r] = z2[8 + r]
        M[ta, 1 + r] = m2[10 + r]
    M[ta, 3 - 3 * ta] = m1[10 + ta]
    M[ta, 3 * ta] = z1[11 - ta]
    M[other, 3 * ta] = z2[11 - ta]
    for r in range(4):
        A[other, r + 2 - 2 * ta] = oc[0, r]
    for k in range(3):
        M[other, k + 1 - ta] = oc[1, k + ta]
    for e in range(6):
        C[4, e] = jnp.zeros(m1.shape[1:], bf16)
        C[5, e] = jnp.zeros(m1.shape[1:], bf16)
    partial_products(ws, AC, PV, ta)


def shifted_sum(p, edge_ref, q):
    lane = lanes_of(p[1].shape)
    amount = (126 - q) % 128 if isinstance(q, int) else lax.rem(254 - q, 128)
    back = pltpu.roll(edge_ref[...], amount, 1)
    out = p[1] + jnp.where(lane == 0, back, pltpu.roll(p[0], 1, 1))
    return out + jnp.where(lane == 127, back, pltpu.roll(p[2], 127, 1))


def second_products(f, M, D, w2, w1f):
    return parts(product(w2[...], M, (), f, 0)), parts(product(w1f[...], D, (), f, 0))


def second_layer(f, mine, slot, out, both, PA, PC, vec):
    pf, pb = both
    for i in range(2):
        q = f * 32 + i * 4
        frame = mine[2 * slot + i].astype(f32)
        cot = mine[4 + 2 * slot + i].astype(f32)
        decoded = frame + (shifted_sum(pf[i], PA, q) + vec[3])
        out[0, slot, i] = decoded.astype(bf16).astype(f32)
        _, back = act_and_back(frame, vec[0], shifted_sum(pb[i], PC, q))
        out[1, slot, i] = cot + back


def own_body(m2, M, D, PA, PC, w2, w1f, vec, keep):
    ta = lax.axis_index("ta")
    for slot in range(2):
        f = 2 * ta + slot
        second_layer(f, m2, slot, keep, second_products(f, M, D, w2, w1f), PA, PC, vec)


def main_body(
    AC_in, M_in, PV_in, sp, edge, e1, e2, ws, w2, w1f, vec,
    AC, M, PV, D, PA, PC, send, EA, EC,
):
    A, C, w1, w2f = AC.at[0], AC.at[1], ws.at[0], ws.at[1]
    channels = sp.shape[1]
    tile = (channels, 128)
    ta, other, _, mb = offsets()
    ha = lax.axis_index("ha")
    wa = lax.axis_index("wa")
    first_row = (ta == 1) | (ha > 0)
    last_row = (ta == 0) | (ha < lax.axis_size("ha") - 1)
    left_col = wa > 0
    right_col = wa < lax.axis_size("wa") - 1
    lane = lanes_of(tile)
    column = lane % 4
    gin, gmid, bin_, _ = (vec[k] for k in range(4))

    for i in range(2):
        for r in range(2):
            for src, at, frame, row in (
                (sp, 2 * i + r, 2 * other + i, 2 + r),
                (sp, 8 + 2 * i + r, 2 * other + i, mb + r),
            ):
                A[2 + frame, row] = act(src[at].astype(f32), gin).astype(bf16)
                C[frame, row] = src[at + 4]
    for e in range(4):
        D[4, e] = jnp.zeros(tile, bf16)
        D[5, e] = jnp.zeros(tile, bf16)

    own, par, zo, zp = (t[...].astype(f32) for t in (edge, sp.at[16], e1, e2))

    def placed(t, slot, start, rows_from, rows, to):
        moved = pltpu.roll(t, (start + 4 * to - 16 * slot - 4 * rows_from) % 128, 1)
        low = start + 4 * to
        return jnp.where((lane >= low) & (lane < low + 4 * rows), moved, 0.0)

    def group(first):
        mine = yours = 0.0
        for i in range(2):
            mine += placed(own, first + i, 32 * i, 0, 4, 2 - 2 * ta)
            mine += placed(zo, first + i, 32 * i, 2 - 2 * ta, 2, 4 * ta)
            yours += placed(par, first + i, 32 * i, 0, 4, 2 - 2 * ta)
            yours += placed(zp, first + i, 32 * i, 2 - 2 * ta, 2, 4 * ta)
        g0 = jnp.where(ta == 0, mine, yours)
        g1 = jnp.where(ta == 0, yours, mine)
        return g0 + pltpu.roll(g1, 64, 1)

    def caches(slot):
        out = placed(own, slot, 32 * ta, 0, 4, 2 - 2 * ta)
        out += placed(zo, slot, 32 * ta, 2 - 2 * ta, 2, 4 * ta)
        out += placed(par, slot, 32 * other, 0, 4, 2 - 2 * ta)
        return out + placed(zp, slot, 32 * other, 2 - 2 * ta, 2, 4 * ta)

    def edge_products(w, low, high, last=False):
        pieces = []
        for t, a in taps_order:
            s = 32 * t + 4 * a
            if s == 0:
                pieces.append(low.astype(bf16))
                continue
            moved = pltpu.roll(low, 128 - s, 1)
            beyond = 0.0 if high is None else pltpu.roll(high, 128 - s, 1)
            pieces.append(jnp.where(lane < 128 - s, moved, beyond).astype(bf16))
        stacked = jnp.concatenate(pieces, axis=0)
        if last:
            outer = jnp.concatenate([w[:channels, :], w[2 * channels :, :]], axis=0)
            p = jnp.dot(outer, stacked, preferred_element_type=f32)
            return jnp.where(column == 2, p[:channels], p[channels:])
        p = jnp.dot(w[...], stacked, preferred_element_type=f32)
        p0, p1, p2 = (p[b * channels : (b + 1) * channels] for b in range(3))
        across = jnp.where(column == 2, p0, p2)
        own_part = jnp.where(column == 2, pltpu.roll(p0, 127, 1), pltpu.roll(p2, 1, 1)) + p1
        return across, own_part

    def to_edges(p, edge_ref, q):
        moved = pltpu.roll(jnp.where(lane == 0, p[2], p[0]), q + 2, 1)
        here = (lane == q + 1) | (lane == q + 2)
        edge_ref[...] = edge_ref[...] + jnp.where(here, moved, 0.0)

    def first_products(f, pair):
        forward = PV[0, f, pair] if f < 2 else product(w1[...], A, (), f, 2 * pair)
        gradient = PV[1, f - 2, pair] if f > 1 else product(w2f[...], C, (), f, 2 * pair)
        return parts(forward), parts(gradient)

    partial_products(ws, AC, PV, other)
    act_edges = pltpu.roll(act(group(0), gin), 64, 1)
    cin_edges = caches(4)
    across, own_part = edge_products(
        w1, jnp.where(lane < 64, cin_edges, act_edges), jnp.where(lane < 64, act_edges, 0.0)
    )
    PA[...] = across
    EA[...] = own_part
    across, own_part = edge_products(w2f, group(2), None)
    PC[...] = across
    EC[...] = own_part
    cmid_edges = pltpu.roll(caches(5), 124, 1)

    def first_layer(f):
        for pair in range(2):
            pf, pb = first_products(f, pair)
            for i in range(2):
                e = 2 * pair + i
                q = f * 32 + e * 4
                hidden = (shifted_sum(pf[i], PA, q) + bin_).astype(bf16).astype(f32)
                back = shifted_sum(pb[i], PC, q)
                to_edges(pf[i], EA, q)
                to_edges(pb[i], EC, q)
                a, d = act_and_back(hidden, gmid, back)
                if e == 0:
                    a = jnp.where(first_row, a, 0.0)
                    d = jnp.where(first_row, d, 0.0)
                if e == 3:
                    a = jnp.where(last_row, a, 0.0)
                    d = jnp.where(last_row, d, 0.0)
                M[2 + f, e] = a.astype(bf16)
                D[f, e] = d.astype(bf16)

    for f in range(4):
        first_layer(f)

    late = [second_products(2 * other + slot, M, D, w2, w1f) for slot in range(2)]
    hidden = (EA[...] + bin_).astype(bf16).astype(f32)
    a, d = act_and_back(hidden, gmid, EC[...])
    row = (lane % 32) // 4
    inside = ((column == 2) & left_col) | ((column == 1) & right_col)
    inside = inside & (row < 4) & ((row > 0) | first_row) & ((row < 3) | last_row)
    a = jnp.where(inside, a, 0.0).astype(bf16).astype(f32)
    d = jnp.where(inside, d, 0.0).astype(bf16).astype(f32)
    a = pltpu.roll(a, 64, 1)
    low = jnp.where(lane < 64, cmid_edges, a)
    PA[...] = edge_products(w2, low, jnp.where(lane < 64, a, 0.0), last=True)
    PC[...] = edge_products(w1f, d, None, last=True)

    for slot in range(2):
        second_layer(2 * other + slot, sp, slot, send, late[slot], PA, PC, vec)


def assemble_body(keep, got, dec, grad, scr):
    channels = got.shape[3]
    flat = 4 * channels
    ta = lax.axis_index("ta")

    def write(at_keep, at_got):
        for f in range(2):
            for i in range(2):
                for src, r in ((keep, at_keep + i), (got, at_got + i)):
                    scr[pl.ds(f * flat + r, channels, stride=4), :] = src[0, f, i]
                    grad[pl.ds(f * flat + r, channels, stride=4), :] = src[1, f, i]

    @pl.when(ta == 0)
    def _():
        write(0, 2)

    @pl.when(ta == 1)
    def _():
        write(2, 0)

    dec[...] = scr[...].astype(bf16)


def per_device(
    frames, cache_in, cache_mid, gain_in, gain_mid,
    weight_in, bias_in, weight_mid, bias_mid, cotangent,
):
    n, c, height, width = frames.shape
    flat = lambda v: v.reshape(n * c * height, width)
    tile = (c, width)
    limit = lambda mib: pltpu.CompilerParams(vmem_limit_bytes=mib << 20)
    row = lambda v: v.reshape(1, c)
    taps = lambda w: w.reshape(3, 3 * c, 3 * c)
    ed, scr, rows = pl.pallas_call(
        fetch_body,
        in_specs=[HB] * 8,
        out_specs=(VM,) * 3,
        out_shape=(
            pltpu.VMEM(tile, bf16),
            pltpu.VMEM((8, c * height, width), f32),
            pltpu.VMEM((4, 1, c), f32),
        ),
        scratch_shapes=[
            pltpu.VMEM((4, n * c * height, width), bf16),
            pltpu.SemaphoreType.DMA((16,)),
            pltpu.SemaphoreType.DMA((4,)),
        ],
        compiler_params=limit(6),
        name="fetch",
    )(
        *far(
            flat(frames), flat(cotangent), flat(cache_in), flat(cache_mid),
            row(gain_in), row(gain_mid), row(bias_in), row(bias_mid),
        )
    )
    wi, wm = near(taps(weight_in), taps(weight_mid))
    m1, m2, oc, sw = pl.pallas_call(
        pack_body,
        in_specs=[VM] * 2,
        out_specs=(VM,) * 4,
        out_shape=(
            pltpu.VMEM((12,) + tile, bf16),
            pltpu.VMEM((12,) + tile, bf16),
            pltpu.VMEM((2, 4) + tile, bf16),
            pltpu.VMEM((17,) + tile, bf16),
        ),
        compiler_params=limit(4),
        name="pack",
    )(*near(scr, wi))

    wide = lax.axis_size("wa")
    high = lax.axis_size("ha")
    pairs = lambda start: [
        p for i in range(start, wide - 1, 2) for p in ((i, i + 1), (i + 1, i))
    ]
    one = [(2 * i, 2 * i + 2) for i in range(high - 1)]
    one += [(2 * i + 3, 2 * i + 1) for i in range(high - 1)]
    two = [(2 * i + 2, 2 * i + 1) for i in range(high - 1)]
    two += [(2 * i + 1, 2 * i + 2) for i in range(high - 1)]
    second = lax.ppermute(ed, "wa", pairs(1))
    first = lax.ppermute(ed, "wa", pairs(0))
    z1 = lax.ppermute(m1, ("ha", "ta"), one)
    z2 = lax.ppermute(m2, ("ha", "ta"), two)
    sw, edge = pl.pallas_call(
        merge_body,
        in_specs=[VM] * 3,
        out_specs=(VM,) * 2,
        out_shape=(pltpu.VMEM((17,) + tile, bf16), pltpu.VMEM(tile, bf16)),
        input_output_aliases={2: 0},
        compiler_params=limit(2),
        name="merge",
    )(*near(first, second, sw))
    sp = lax.ppermute(sw, "ta", [(0, 1), (1, 0)])
    e1 = lax.ppermute(edge, ("ha", "ta"), one)
    e2 = lax.ppermute(edge, ("ha", "ta"), two)

    matrix = pltpu.VMEM((3 * c, 9 * c), bf16)
    ws, w2, w1f, vec = pl.pallas_call(
        weights_body,
        in_specs=[VM] * 3 + [pl.BlockSpec(memory_space=pl.ANY)],
        out_specs=(VM,) * 4,
        out_shape=(
            pltpu.VMEM((2, 3 * c, 9 * c), bf16),
            matrix,
            matrix,
            pltpu.VMEM((4,) + tile, f32),
        ),
        compiler_params=limit(8),
        name="weights",
    )(*near(wi, wm, rows), m2)
    staged = (
        pltpu.VMEM((2, 6, 6) + tile, bf16),
        pltpu.VMEM((6, 4) + tile, bf16),
        pltpu.VMEM((2, 2, 2, 3 * c, 2 * width), f32),
    )
    AC, M, PV = pl.pallas_call(
        lead_body,
        in_specs=[VM] * 7,
        out_specs=(VM,) * 3,
        out_shape=staged,
        compiler_params=limit(8),
        name="lead",
    )(*near(m1, m2, oc, z1, z2, vec, ws))
    half = pltpu.VMEM((2, 2, 2) + tile, f32)
    AC, M, PV, D, PA, PC, send = pl.pallas_call(
        main_body,
        in_specs=[VM] * 11,
        out_specs=(VM,) * 7,
        out_shape=staged
        + (
            pltpu.VMEM((6, 4) + tile, bf16),
            pltpu.VMEM(tile, f32),
            pltpu.VMEM(tile, f32),
            half,
        ),
        scratch_shapes=[pltpu.VMEM(tile, f32), pltpu.VMEM(tile, f32)],
        input_output_aliases={0: 0, 1: 1, 2: 2},
        compiler_params=limit(12),
        name="block",
    )(*near(AC, M, PV, sp, edge, e1, e2, ws, w2, w1f, vec))
    got = lax.ppermute(send, "ta", [(0, 1), (1, 0)])
    keep = pl.pallas_call(
        own_body,
        in_specs=[VM] * 8,
        out_specs=VM,
        out_shape=half,
        compiler_params=limit(8),
        name="own",
    )(*near(m2, M, D, PA, PC, w2, w1f, vec))
    decoded, grad = pl.pallas_call(
        assemble_body,
        in_specs=[VM] * 2,
        out_shape=(
            jax.ShapeDtypeStruct((n * c * height, width), bf16),
            jax.ShapeDtypeStruct((n * c * height, width), f32),
        ),
        scratch_shapes=[pltpu.VMEM((n * c * height, width), f32)],
        compiler_params=limit(8),
        name="assemble",
    )(*near(keep, got))
    return decoded.reshape(frames.shape), grad.reshape(frames.shape)


def solution(mesh):
    split = P(("grp", "ta"), None, "ha", "wa")
    cache = P("grp", None, "ha", "wa")
    return jax.shard_map(
        per_device,
        mesh=mesh,
        in_specs=(split, cache, cache, P(), P(), P(), P(), P(), P(), split),
        out_specs=(split, split),
        check_vma=False,
    )
```

```python
import jax
import jax.numpy as jnp
from jax import lax
from jax.experimental import pallas as pl
from jax.experimental.pallas import tpu as pltpu
from jax.sharding import PartitionSpec as P


epsilon = 1e-06
f32 = jnp.float32
bf16 = jnp.bfloat16
VM = pl.BlockSpec(memory_space=pltpu.VMEM)
HB = pl.BlockSpec(memory_space=pltpu.HBM)


def near(*values):
    return [pltpu.with_memory_space_constraint(v, pltpu.VMEM) for v in values]


def far(*values):
    return [pltpu.with_memory_space_constraint(v, pltpu.HBM) for v in values]


def lanes_of(shape):
    return lax.broadcasted_iota(jnp.int32, shape, len(shape) - 1)


def act(v, g):
    r = lax.rsqrt(jnp.mean(v * v, axis=0, keepdims=True) + epsilon)
    z = v * r * g
    return z * jax.nn.sigmoid(z)


def act_and_back(v, g, d):
    r = lax.rsqrt(jnp.mean(v * v, axis=0, keepdims=True) + epsilon)
    vr = v * r
    z = vr * g
    s = jax.nn.sigmoid(z)
    q = g * d * s * (1.0 + z * (1.0 - s))
    back = r * q - vr * (r * r) * jnp.mean(q * v, axis=0, keepdims=True)
    return z * s, back


def fetch_body(
    fr_far, ct_far, ci_far, cm_far, wm_far, gi, gm, bi, bm,
    ed, scr, wm, rows_of, inp, sems, others,
):
    channels = ed.shape[0]
    rows = 4
    flat = channels * rows
    half = flat // 2
    ta = lax.axis_index("ta")
    own = pl.multiple_of(ta * flat, flat)
    other = pl.multiple_of((1 - ta) * flat, flat)
    starts = [(fr_far, 0), (fr_far, flat), (ct_far, 0), (ct_far, flat)]
    starts += [(ci_far, own), (cm_far, own), (ci_far, other), (cm_far, other)]
    copies = [
        [
            pltpu.make_async_copy(
                source.at[pl.ds(start + k * half, half)],
                inp.at[s, pl.ds(k * half, half)],
                sems.at[2 * s + k],
            )
            for k in range(2)
        ]
        for s, (source, start) in enumerate(starts)
    ]
    rest = [pltpu.make_async_copy(wm_far, wm, others.at[4])]
    rest += [
        pltpu.make_async_copy(source, rows_of.at[k], others.at[k])
        for k, source in enumerate((gi, gm, bi, bm))
    ]
    for group in copies + [rest]:
        for copy in group:
            copy.start()
    k = lax.broadcasted_iota(jnp.int32, (rows * 128, 128), 0)
    j = lanes_of((rows * 128, 128))
    column = jnp.where(j % 4 == 0, 1, jnp.where(j % 4 == 1, 0, jnp.where(j % 4 == 2, 127, 126)))
    chosen = (j < 4 * rows) & (k // 128 == j // 4) & (k % 128 == column)
    chosen = jnp.where(chosen, 1.0, 0.0).astype(bf16)
    edges = jnp.zeros((channels, 128), f32)
    for s in range(6):
        for copy in copies[s]:
            copy.wait()
        scr[s] = inp[s].astype(f32)
    for s in range(6):
        tiles = [scr[s, pl.ds(r, channels, stride=rows), :].astype(bf16) for r in range(rows)]
        part = jnp.dot(jnp.concatenate(tiles, axis=1), chosen, preferred_element_type=f32)
        edges = edges + (pltpu.roll(part, 4 * rows * s, 1) if s else part)
    ed[...] = edges.astype(bf16)
    for s in (6, 7):
        for copy in copies[s]:
            copy.wait()
        scr[s] = inp[s].astype(f32)
    for copy in rest:
        copy.wait()


def pack_body(scr, m1, m2, oc, sw):
    channels = m1.shape[1]
    ta = lax.axis_index("ta")
    tile_of = lambda s, r: scr[s, pl.ds(r, channels, stride=4), :].astype(bf16)
    for s in range(6):
        for i in range(2):
            far_half = tile_of(s, 2 - 2 * ta + i)
            own_half = tile_of(s, 2 * ta + i)
            m1[2 * s + i] = far_half
            m2[2 * s + i] = own_half
            if s < 4:
                sw[2 * s + i] = far_half
                sw[8 + 2 * s + i] = own_half
    for s in range(2):
        for r in range(4):
            oc[s, r] = tile_of(6 + s, r)


def merge_body(first, second, sw_in, sw, edge_out):
    even = lax.rem(lax.axis_index("wa"), 2) == 0
    a, b = first[...].astype(f32), second[...].astype(f32)
    inner = lanes_of(a.shape) % 4 >= 2
    edge = jnp.where(inner == even, b, a).astype(bf16)
    edge_out[...] = edge
    sw[16] = edge


def weights_body(win, wmid, rows, after, ws, w2, w1f, vec):
    channels = w2.shape[0] // 3
    w1, w2f = ws.at[0], ws.at[1]
    for src, plain, turned in zip((win, wmid), (w1, w2), (w1f, w2f)):
        plain[...] = jnp.concatenate([src[a].astype(f32) for a in range(3)], axis=1).astype(bf16)
        for b in range(3):
            flat = [
                jnp.transpose(src[2 - a, (2 - b) * channels : (3 - b) * channels, :].astype(f32))
                for a in range(3)
            ]
            blocks = [
                flat[a][(2 - t) * channels : (3 - t) * channels] for a in range(3) for t in range(3)
            ]
            turned[b * channels : (b + 1) * channels, :] = jnp.concatenate(blocks, axis=1).astype(
                bf16
            )
    for k in range(4):
        vec[k] = jnp.transpose(jnp.broadcast_to(rows[k], (128, channels)))


def offsets():
    ta = lax.axis_index("ta")
    return ta, 1 - ta, 4 * ta, 4 - 4 * ta


taps_order = [(t, a) for a in range(3) for t in range(3)]


def product(weights, ref, lead, f, row):
    cols = [
        jnp.concatenate([ref[lead + (f + t, row + i + a)] for t, a in taps_order], axis=0)
        for i in range(2)
    ]
    return jnp.dot(weights, jnp.concatenate(cols, axis=1), preferred_element_type=f32)


def parts(p):
    n = p.shape[0] // 3
    return [[p[b * n : (b + 1) * n, 128 * i : 128 * (i + 1)] for b in range(3)] for i in range(2)]


def partial_products(ws, AC, PV, which):
    for k in range(2):
        for pair in range(2):
            PV[which, k, pair] = product(ws[which], AC, (which,), 2 * which + k, 2 * pair)


def lead_body(m1, m2, oc, z1, z2, vec, ws, AC, M, PV):
    A, C = AC.at[0], AC.at[1]
    ta, other, zb, mb = offsets()
    gin = vec[0]
    for i in range(2):
        for r in range(2):
            at = 2 * i + r
            for src, frame, row in (
                (m2, 2 * ta + i, 2 + r),
                (m1, 2 * ta + i, mb + r),
                (z1, 2 * ta + i, zb + r),
                (z2, 2 * other + i, zb + r),
            ):
                A[2 + frame, row] = act(src[at].astype(f32), gin).astype(bf16)
                C[frame, row] = src[at + 4]
    for r in range(2):
        A[ta, 2 + r] = m2[8 + r]
        A[ta, mb + r] = m1[8 + r]
        A[ta, zb + r] = z1[8 + r]
        A[other, zb + r] = z2[8 + r]
        M[ta, 1 + r] = m2[10 + r]
    M[ta, 3 - 3 * ta] = m1[10 + ta]
    M[ta, 3 * ta] = z1[11 - ta]
    M[other, 3 * ta] = z2[11 - ta]
    for r in range(4):
        A[other, r + 2 - 2 * ta] = oc[0, r]
    for k in range(3):
        M[other, k + 1 - ta] = oc[1, k + ta]
    for e in range(6):
        C[4, e] = jnp.zeros(m1.shape[1:], bf16)
        C[5, e] = jnp.zeros(m1.shape[1:], bf16)
    partial_products(ws, AC, PV, ta)


def shifted_sum(p, edge_ref, q):
    lane = lanes_of(p[1].shape)
    amount = (126 - q) % 128 if isinstance(q, int) else lax.rem(254 - q, 128)
    back = pltpu.roll(edge_ref[...], amount, 1)
    out = p[1] + jnp.where(lane == 0, back, pltpu.roll(p[0], 1, 1))
    return out + jnp.where(lane == 127, back, pltpu.roll(p[2], 127, 1))


def second_products(f, M, D, w2, w1f):
    return parts(product(w2[...], M, (), f, 0)), parts(product(w1f[...], D, (), f, 0))


def second_layer(f, mine, slot, out, both, PA, PC, vec, whole):
    pf, pb = both
    for i in range(2):
        q = f * 32 + i * 4
        frame = mine[2 * slot + i].astype(f32)
        cot = mine[4 + 2 * slot + i].astype(f32) if whole else None
        decoded = frame + (shifted_sum(pf[i], PA, q) + vec[3])
        out[0, slot, i] = decoded.astype(bf16).astype(out.dtype)
        _, back = act_and_back(frame, vec[0], shifted_sum(pb[i], PC, q))
        out[1, slot, i] = cot + back if whole else back.astype(out.dtype)


def own_body(m2, M, D, PA, PC, w2, w1f, vec, keep):
    ta = lax.axis_index("ta")
    for slot in range(2):
        f = 2 * ta + slot
        second_layer(f, m2, slot, keep, second_products(f, M, D, w2, w1f), PA, PC, vec, True)


def main_body(
    AC_in, M_in, PV_in, sp, edge, e1, e2, ws, w2, w1f, vec,
    AC, M, PV, D, PA, PC, send, EA, EC,
):
    A, C, w1, w2f = AC.at[0], AC.at[1], ws.at[0], ws.at[1]
    channels = sp.shape[1]
    tile = (channels, 128)
    ta, other, _, mb = offsets()
    ha = lax.axis_index("ha")
    wa = lax.axis_index("wa")
    first_row = (ta == 1) | (ha > 0)
    last_row = (ta == 0) | (ha < lax.axis_size("ha") - 1)
    left_col = wa > 0
    right_col = wa < lax.axis_size("wa") - 1
    lane = lanes_of(tile)
    column = lane % 4
    gin, gmid, bin_, _ = (vec[k] for k in range(4))

    for i in range(2):
        for r in range(2):
            for src, at, frame, row in (
                (sp, 2 * i + r, 2 * other + i, 2 + r),
                (sp, 8 + 2 * i + r, 2 * other + i, mb + r),
            ):
                A[2 + frame, row] = act(src[at].astype(f32), gin).astype(bf16)
                C[frame, row] = src[at + 4]
    for e in range(4):
        D[4, e] = jnp.zeros(tile, bf16)
        D[5, e] = jnp.zeros(tile, bf16)

    own, par, zo, zp = (t[...].astype(f32) for t in (edge, sp.at[16], e1, e2))

    def placed(t, slot, start, rows_from, rows, to):
        moved = pltpu.roll(t, (start + 4 * to - 16 * slot - 4 * rows_from) % 128, 1)
        low = start + 4 * to
        return jnp.where((lane >= low) & (lane < low + 4 * rows), moved, 0.0)

    def group(first):
        mine = yours = 0.0
        for i in range(2):
            mine += placed(own, first + i, 32 * i, 0, 4, 2 - 2 * ta)
            mine += placed(zo, first + i, 32 * i, 2 - 2 * ta, 2, 4 * ta)
            yours += placed(par, first + i, 32 * i, 0, 4, 2 - 2 * ta)
            yours += placed(zp, first + i, 32 * i, 2 - 2 * ta, 2, 4 * ta)
        g0 = jnp.where(ta == 0, mine, yours)
        g1 = jnp.where(ta == 0, yours, mine)
        return g0 + pltpu.roll(g1, 64, 1)

    def caches(slot):
        out = placed(own, slot, 32 * ta, 0, 4, 2 - 2 * ta)
        out += placed(zo, slot, 32 * ta, 2 - 2 * ta, 2, 4 * ta)
        out += placed(par, slot, 32 * other, 0, 4, 2 - 2 * ta)
        return out + placed(zp, slot, 32 * other, 2 - 2 * ta, 2, 4 * ta)

    def edge_products(w, low, high, last=False):
        pieces = []
        for t, a in taps_order:
            s = 32 * t + 4 * a
            if s == 0:
                pieces.append(low.astype(bf16))
                continue
            moved = pltpu.roll(low, 128 - s, 1)
            beyond = 0.0 if high is None else pltpu.roll(high, 128 - s, 1)
            pieces.append(jnp.where(lane < 128 - s, moved, beyond).astype(bf16))
        stacked = jnp.concatenate(pieces, axis=0)
        if last:
            outer = jnp.concatenate([w[:channels, :], w[2 * channels :, :]], axis=0)
            p = jnp.dot(outer, stacked, preferred_element_type=f32)
            return jnp.where(column == 2, p[:channels], p[channels:])
        p = jnp.dot(w[...], stacked, preferred_element_type=f32)
        p0, p1, p2 = (p[b * channels : (b + 1) * channels] for b in range(3))
        across = jnp.where(column == 2, p0, p2)
        own_part = jnp.where(column == 2, pltpu.roll(p0, 127, 1), pltpu.roll(p2, 1, 1)) + p1
        return across, own_part

    def to_edges(p, edge_ref, q):
        moved = pltpu.roll(jnp.where(lane == 0, p[2], p[0]), q + 2, 1)
        here = (lane == q + 1) | (lane == q + 2)
        edge_ref[...] = edge_ref[...] + jnp.where(here, moved, 0.0)

    def first_products(f, pair):
        forward = PV[0, f, pair] if f < 2 else product(w1[...], A, (), f, 2 * pair)
        gradient = PV[1, f - 2, pair] if f > 1 else product(w2f[...], C, (), f, 2 * pair)
        return parts(forward), parts(gradient)

    partial_products(ws, AC, PV, other)
    act_edges = pltpu.roll(act(group(0), gin), 64, 1)
    cin_edges = caches(4)
    across, own_part = edge_products(
        w1, jnp.where(lane < 64, cin_edges, act_edges), jnp.where(lane < 64, act_edges, 0.0)
    )
    PA[...] = across
    EA[...] = own_part
    across, own_part = edge_products(w2f, group(2), None)
    PC[...] = across
    EC[...] = own_part
    cmid_edges = pltpu.roll(caches(5), 124, 1)

    def first_layer(f):
        for pair in range(2):
            pf, pb = first_products(f, pair)
            for i in range(2):
                e = 2 * pair + i
                q = f * 32 + e * 4
                hidden = (shifted_sum(pf[i], PA, q) + bin_).astype(bf16).astype(f32)
                back = shifted_sum(pb[i], PC, q)
                to_edges(pf[i], EA, q)
                to_edges(pb[i], EC, q)
                a, d = act_and_back(hidden, gmid, back)
                if e == 0:
                    a = jnp.where(first_row, a, 0.0)
                    d = jnp.where(first_row, d, 0.0)
                if e == 3:
                    a = jnp.where(last_row, a, 0.0)
                    d = jnp.where(last_row, d, 0.0)
                M[2 + f, e] = a.astype(bf16)
                D[f, e] = d.astype(bf16)

    for f in range(4):
        first_layer(f)

    late = [second_products(2 * other + slot, M, D, w2, w1f) for slot in range(2)]
    hidden = (EA[...] + bin_).astype(bf16).astype(f32)
    a, d = act_and_back(hidden, gmid, EC[...])
    row = (lane % 32) // 4
    inside = ((column == 2) & left_col) | ((column == 1) & right_col)
    inside = inside & (row < 4) & ((row > 0) | first_row) & ((row < 3) | last_row)
    a = jnp.where(inside, a, 0.0).astype(bf16).astype(f32)
    d = jnp.where(inside, d, 0.0).astype(bf16).astype(f32)
    a = pltpu.roll(a, 64, 1)
    low = jnp.where(lane < 64, cmid_edges, a)
    PA[...] = edge_products(w2, low, jnp.where(lane < 64, a, 0.0), last=True)
    PC[...] = edge_products(w1f, d, None, last=True)

    for slot in range(2):
        second_layer(2 * other + slot, sp, slot, send, late[slot], PA, PC, vec, False)


def assemble_body(keep, got, m1, dec, grad, scr):
    channels = keep.shape[3]
    flat = 4 * channels
    ta = lax.axis_index("ta")
    for f in range(2):
        for i in range(2):
            mine = pl.ds(f * flat + 2 * ta + i, channels, stride=4)
            yours = pl.ds(f * flat + 2 - 2 * ta + i, channels, stride=4)
            scr[mine, :] = keep[0, f, i]
            grad[mine, :] = keep[1, f, i]
            scr[yours, :] = got[0, f, i].astype(f32)
            grad[yours, :] = m1[4 + 2 * f + i].astype(f32) + got[1, f, i].astype(f32)
    dec[...] = scr[...].astype(bf16)


def per_device(
    frames, cache_in, cache_mid, gain_in, gain_mid,
    weight_in, bias_in, weight_mid, bias_mid, cotangent,
):
    n, c, height, width = frames.shape
    flat = lambda v: v.reshape(n * c * height, width)
    tile = (c, width)
    limit = lambda mib: pltpu.CompilerParams(vmem_limit_bytes=mib << 20)
    row = lambda v: v.reshape(1, c)
    taps = lambda w: w.reshape(3, 3 * c, 3 * c)
    ed, scr, wm, rows = pl.pallas_call(
        fetch_body,
        in_specs=[HB] * 9,
        out_specs=(VM,) * 4,
        out_shape=(
            pltpu.VMEM(tile, bf16),
            pltpu.VMEM((8, c * height, width), f32),
            pltpu.VMEM((3, 3 * c, 3 * c), bf16),
            pltpu.VMEM((4, 1, c), f32),
        ),
        scratch_shapes=[
            pltpu.VMEM((8, c * height, width), bf16),
            pltpu.SemaphoreType.DMA((16,)),
            pltpu.SemaphoreType.DMA((5,)),
        ],
        compiler_params=limit(6),
        name="fetch",
    )(
        *far(
            flat(frames), flat(cotangent), flat(cache_in), flat(cache_mid),
            taps(weight_mid), row(gain_in), row(gain_mid), row(bias_in), row(bias_mid),
        )
    )
    m1, m2, oc, sw = pl.pallas_call(
        pack_body,
        in_specs=[VM],
        out_specs=(VM,) * 4,
        out_shape=(
            pltpu.VMEM((12,) + tile, bf16),
            pltpu.VMEM((12,) + tile, bf16),
            pltpu.VMEM((2, 4) + tile, bf16),
            pltpu.VMEM((17,) + tile, bf16),
        ),
        compiler_params=limit(4),
        name="pack",
    )(*near(scr))

    wide = lax.axis_size("wa")
    high = lax.axis_size("ha")
    pairs = lambda start: [
        p for i in range(start, wide - 1, 2) for p in ((i, i + 1), (i + 1, i))
    ]
    one = [(2 * i, 2 * i + 2) for i in range(high - 1)]
    one += [(2 * i + 3, 2 * i + 1) for i in range(high - 1)]
    two = [(2 * i + 2, 2 * i + 1) for i in range(high - 1)]
    two += [(2 * i + 1, 2 * i + 2) for i in range(high - 1)]
    second = lax.ppermute(ed, "wa", pairs(1))
    first = lax.ppermute(ed, "wa", pairs(0))
    z1 = lax.ppermute(m1, ("ha", "ta"), one)
    z2 = lax.ppermute(m2, ("ha", "ta"), two)
    sw, edge = pl.pallas_call(
        merge_body,
        in_specs=[VM] * 3,
        out_specs=(VM,) * 2,
        out_shape=(pltpu.VMEM((17,) + tile, bf16), pltpu.VMEM(tile, bf16)),
        input_output_aliases={2: 0},
        compiler_params=limit(2),
        name="merge",
    )(*near(first, second, sw))
    sp = lax.ppermute(sw, "ta", [(0, 1), (1, 0)])
    e1 = lax.ppermute(edge, ("ha", "ta"), one)
    e2 = lax.ppermute(edge, ("ha", "ta"), two)

    matrix = pltpu.VMEM((3 * c, 9 * c), bf16)
    ws, w2, w1f, vec = pl.pallas_call(
        weights_body,
        in_specs=[VM] * 3 + [pl.BlockSpec(memory_space=pl.ANY)],
        out_specs=(VM,) * 4,
        out_shape=(
            pltpu.VMEM((2, 3 * c, 9 * c), bf16),
            matrix,
            matrix,
            pltpu.VMEM((4,) + tile, f32),
        ),
        compiler_params=limit(8),
        name="weights",
    )(*near(taps(weight_in), wm, rows), m2)
    staged = (
        pltpu.VMEM((2, 6, 6) + tile, bf16),
        pltpu.VMEM((6, 4) + tile, bf16),
        pltpu.VMEM((2, 2, 2, 3 * c, 2 * width), f32),
    )
    AC, M, PV = pl.pallas_call(
        lead_body,
        in_specs=[VM] * 7,
        out_specs=(VM,) * 3,
        out_shape=staged,
        compiler_params=limit(8),
        name="lead",
    )(*near(m1, m2, oc, z1, z2, vec, ws))
    half = pltpu.VMEM((2, 2, 2) + tile, f32)
    AC, M, PV, D, PA, PC, send = pl.pallas_call(
        main_body,
        in_specs=[VM] * 11,
        out_specs=(VM,) * 7,
        out_shape=staged
        + (
            pltpu.VMEM((6, 4) + tile, bf16),
            pltpu.VMEM(tile, f32),
            pltpu.VMEM(tile, f32),
            pltpu.VMEM((2, 2, 2) + tile, bf16),
        ),
        scratch_shapes=[pltpu.VMEM(tile, f32), pltpu.VMEM(tile, f32)],
        input_output_aliases={0: 0, 1: 1, 2: 2},
        compiler_params=limit(12),
        name="block",
    )(*near(AC, M, PV, sp, edge, e1, e2, ws, w2, w1f, vec))
    got = lax.ppermute(send, "ta", [(0, 1), (1, 0)])
    keep = pl.pallas_call(
        own_body,
        in_specs=[VM] * 8,
        out_specs=VM,
        out_shape=half,
        compiler_params=limit(8),
        name="own",
    )(*near(m2, M, D, PA, PC, w2, w1f, vec))
    decoded, grad = pl.pallas_call(
        assemble_body,
        in_specs=[VM] * 3,
        out_shape=(
            jax.ShapeDtypeStruct((n * c * height, width), bf16),
            jax.ShapeDtypeStruct((n * c * height, width), f32),
        ),
        scratch_shapes=[pltpu.VMEM((n * c * height, width), f32)],
        compiler_params=limit(8),
        name="assemble",
    )(*near(keep, got, m1))
    return decoded.reshape(frames.shape), grad.reshape(frames.shape)


def solution(mesh):
    split = P(("grp", "ta"), None, "ha", "wa")
    cache = P("grp", None, "ha", "wa")
    return jax.shard_map(
        per_device,
        mesh=mesh,
        in_specs=(split, cache, cache, P(), P(), P(), P(), P(), P(), split),
        out_specs=(split, split),
        check_vma=False,
    )
```

```python
import jax
import jax.numpy as jnp
from jax import lax
from jax.experimental import pallas as pl
from jax.experimental.pallas import tpu as pltpu
from jax.sharding import PartitionSpec as P


epsilon = 1e-06
f32 = jnp.float32
bf16 = jnp.bfloat16
VM = pl.BlockSpec(memory_space=pltpu.VMEM)
HB = pl.BlockSpec(memory_space=pltpu.HBM)


def near(*values):
    return [pltpu.with_memory_space_constraint(v, pltpu.VMEM) for v in values]


def far(*values):
    return [pltpu.with_memory_space_constraint(v, pltpu.HBM) for v in values]


def lanes_of(shape):
    return lax.broadcasted_iota(jnp.int32, shape, len(shape) - 1)


def act(v, g):
    r = lax.rsqrt(jnp.mean(v * v, axis=0, keepdims=True) + epsilon)
    z = v * r * g
    return z * jax.nn.sigmoid(z)


def act_and_back(v, g, d):
    r = lax.rsqrt(jnp.mean(v * v, axis=0, keepdims=True) + epsilon)
    vr = v * r
    z = vr * g
    s = jax.nn.sigmoid(z)
    q = g * d * s * (1.0 + z * (1.0 - s))
    back = r * q - vr * (r * r) * jnp.mean(q * v, axis=0, keepdims=True)
    return z * s, back


def fetch_body(
    fr_far, ct_far, ci_far, cm_far, wm_far, gi, gm, bi, bm,
    ed, scr, wm, rows_of, inp, sems, others,
):
    channels = ed.shape[0]
    rows = 4
    flat = channels * rows
    half = flat // 2
    ta = lax.axis_index("ta")
    own = pl.multiple_of(ta * flat, flat)
    other = pl.multiple_of((1 - ta) * flat, flat)
    starts = [(fr_far, 0), (fr_far, flat), (ct_far, 0), (ct_far, flat)]
    starts += [(ci_far, own), (cm_far, own), (ci_far, other), (cm_far, other)]
    copies = [
        [
            pltpu.make_async_copy(
                source.at[pl.ds(start + k * half, half)],
                inp.at[s, pl.ds(k * half, half)],
                sems.at[2 * s + k],
            )
            for k in range(2)
        ]
        for s, (source, start) in enumerate(starts)
    ]
    rest = [pltpu.make_async_copy(wm_far, wm, others.at[4])]
    rest += [
        pltpu.make_async_copy(source, rows_of.at[k], others.at[k])
        for k, source in enumerate((gi, gm, bi, bm))
    ]
    for group in copies + [rest]:
        for copy in group:
            copy.start()
    k = lax.broadcasted_iota(jnp.int32, (rows * 128, 128), 0)
    j = lanes_of((rows * 128, 128))
    column = jnp.where(j % 4 == 0, 1, jnp.where(j % 4 == 1, 0, jnp.where(j % 4 == 2, 127, 126)))
    chosen = (j < 4 * rows) & (k // 128 == j // 4) & (k % 128 == column)
    chosen = jnp.where(chosen, 1.0, 0.0).astype(bf16)
    edges = jnp.zeros((channels, 128), f32)
    for s in range(6):
        for copy in copies[s]:
            copy.wait()
        scr[s] = inp[s].astype(f32)
    for s in range(6):
        tiles = [scr[s, pl.ds(r, channels, stride=rows), :].astype(bf16) for r in range(rows)]
        part = jnp.dot(jnp.concatenate(tiles, axis=1), chosen, preferred_element_type=f32)
        edges = edges + (pltpu.roll(part, 4 * rows * s, 1) if s else part)
    ed[...] = edges.astype(bf16)
    for s in (6, 7):
        for copy in copies[s]:
            copy.wait()
        scr[s] = inp[s].astype(f32)
    for copy in rest:
        copy.wait()


def pack_body(scr, m1, m2, oc, sw):
    channels = m1.shape[1]
    ta = lax.axis_index("ta")
    tile_of = lambda s, r: scr[s, pl.ds(r, channels, stride=4), :].astype(bf16)
    for s in range(6):
        for i in range(2):
            far_half = tile_of(s, 2 - 2 * ta + i)
            own_half = tile_of(s, 2 * ta + i)
            m1[2 * s + i] = far_half
            m2[2 * s + i] = own_half
            if s < 4:
                sw[2 * s + i] = far_half
                sw[8 + 2 * s + i] = own_half
    for s in range(2):
        for r in range(4):
            oc[s, r] = tile_of(6 + s, r)


def merge_body(first, second, sw_in, sw, edge_out):
    even = lax.rem(lax.axis_index("wa"), 2) == 0
    a, b = first[...].astype(f32), second[...].astype(f32)
    inner = lanes_of(a.shape) % 4 >= 2
    edge = jnp.where(inner == even, b, a).astype(bf16)
    edge_out[...] = edge
    sw[16] = edge


def weights_body(win, wmid, rows, after, ws, w2, w1f, vec):
    channels = w2.shape[0] // 3
    w1, w2f = ws.at[0], ws.at[1]
    for src, plain, turned in zip((win, wmid), (w1, w2), (w1f, w2f)):
        plain[...] = jnp.concatenate([src[a].astype(f32) for a in range(3)], axis=1).astype(bf16)
        for b in range(3):
            flat = [
                jnp.transpose(src[2 - a, (2 - b) * channels : (3 - b) * channels, :].astype(f32))
                for a in range(3)
            ]
            blocks = [
                flat[a][(2 - t) * channels : (3 - t) * channels] for t in range(3) for a in range(3)
            ]
            turned[b * channels : (b + 1) * channels, :] = jnp.concatenate(blocks, axis=1).astype(
                bf16
            )
    for k in range(4):
        vec[k] = jnp.transpose(jnp.broadcast_to(rows[k], (128, channels)))


def per_core(body):
    def run(*refs):
        index = lax.axis_index("ta")
        for core in range(2):
            pl.when(index == core)(lambda: body(core, *refs))

    return run


def offsets(ta):
    return ta, 1 - ta, 4 * ta, 4 - 4 * ta


forward_order = [(t, a) for a in range(3) for t in range(3)]
gradient_order = [(t, a) for t in range(3) for a in range(3)]


def gradient_taps(f):
    return gradient_order[: 3 * min(3, 4 - f)]


def product(weights, ref, lead, f, row, order):
    cols = [
        jnp.concatenate([ref[lead + (f + t, row + i + a)] for t, a in order], axis=0)
        for i in range(2)
    ]
    weights = weights[:, : cols[0].shape[0]]
    return jnp.dot(weights, jnp.concatenate(cols, axis=1), preferred_element_type=f32)


def parts(p):
    n = p.shape[0] // 3
    return [[p[b * n : (b + 1) * n, 128 * i : 128 * (i + 1)] for b in range(3)] for i in range(2)]


def partial_products(ws, AC, PV, which):
    for k in range(2):
        for pair in range(2):
            f = 2 * which + k
            order = gradient_taps(f) if which else forward_order
            PV[which, k, pair] = product(ws[which], AC, (which,), f, 2 * pair, order)


def lead_body(core, m1, m2, oc, z1, z2, vec, ws, AC, M, PV):
    A, C = AC.at[0], AC.at[1]
    ta, other, zb, mb = offsets(core)
    gin = vec[0]
    for i in range(2):
        for r in range(2):
            at = 2 * i + r
            for src, frame, row in (
                (m2, 2 * ta + i, 2 + r),
                (m1, 2 * ta + i, mb + r),
                (z1, 2 * ta + i, zb + r),
                (z2, 2 * other + i, zb + r),
            ):
                A[2 + frame, row] = act(src[at].astype(f32), gin).astype(bf16)
                C[frame, row] = src[at + 4]
    for r in range(2):
        A[ta, 2 + r] = m2[8 + r]
        A[ta, mb + r] = m1[8 + r]
        A[ta, zb + r] = z1[8 + r]
        A[other, zb + r] = z2[8 + r]
        M[ta, 1 + r] = m2[10 + r]
    M[ta, 3 - 3 * ta] = m1[10 + ta]
    M[ta, 3 * ta] = z1[11 - ta]
    M[other, 3 * ta] = z2[11 - ta]
    for r in range(4):
        A[other, r + 2 - 2 * ta] = oc[0, r]
    for k in range(3):
        M[other, k + 1 - ta] = oc[1, k + ta]
    partial_products(ws, AC, PV, ta)


def shifted_sum(p, edge_ref, q):
    lane = lanes_of(p[1].shape)
    amount = (126 - q) % 128 if isinstance(q, int) else lax.rem(254 - q, 128)
    back = pltpu.roll(edge_ref[...], amount, 1)
    out = p[1] + jnp.where(lane == 0, back, pltpu.roll(p[0], 1, 1))
    return out + jnp.where(lane == 127, back, pltpu.roll(p[2], 127, 1))


def second_products(f, M, D, w2, w1f):
    forward = product(w2[...], M, (), f, 0, forward_order)
    return parts(forward), parts(product(w1f[...], D, (), f, 0, gradient_taps(f)))


def second_layer(f, mine, slot, out, both, PA, PC, vec, whole):
    pf, pb = both
    for i in range(2):
        q = f * 32 + i * 4
        frame = mine[2 * slot + i].astype(f32)
        cot = mine[4 + 2 * slot + i].astype(f32) if whole else None
        decoded = frame + (shifted_sum(pf[i], PA, q) + vec[3])
        out[0, slot, i] = decoded.astype(bf16).astype(out.dtype)
        _, back = act_and_back(frame, vec[0], shifted_sum(pb[i], PC, q))
        out[1, slot, i] = cot + back if whole else back.astype(out.dtype)


def own_body(core, m2, M, D, PA, PC, w2, w1f, vec, keep):
    ta = core
    for slot in range(2):
        f = 2 * ta + slot
        second_layer(f, m2, slot, keep, second_products(f, M, D, w2, w1f), PA, PC, vec, True)


def main_body(
    core, AC_in, M_in, PV_in, sp, edge, e1, e2, ws, w2, w1f, vec,
    AC, M, PV, D, PA, PC, send, EA, EC,
):
    A, C, w1, w2f = AC.at[0], AC.at[1], ws.at[0], ws.at[1]
    channels = sp.shape[1]
    tile = (channels, 128)
    ta, other, _, mb = offsets(core)
    ha = lax.axis_index("ha")
    wa = lax.axis_index("wa")
    first_row = (ta == 1) | (ha > 0)
    last_row = (ta == 0) | (ha < lax.axis_size("ha") - 1)
    left_col = wa > 0
    right_col = wa < lax.axis_size("wa") - 1
    lane = lanes_of(tile)
    column = lane % 4
    gin, gmid, bin_, _ = (vec[k] for k in range(4))

    for i in range(2):
        for r in range(2):
            for src, at, frame, row in (
                (sp, 2 * i + r, 2 * other + i, 2 + r),
                (sp, 8 + 2 * i + r, 2 * other + i, mb + r),
            ):
                A[2 + frame, row] = act(src[at].astype(f32), gin).astype(bf16)
                C[frame, row] = src[at + 4]
    own, par, zo, zp = (t[...].astype(f32) for t in (edge, sp.at[16], e1, e2))

    def placed(t, slot, start, rows_from, rows, to):
        moved = pltpu.roll(t, (start + 4 * to - 16 * slot - 4 * rows_from) % 128, 1)
        low = start + 4 * to
        return jnp.where((lane >= low) & (lane < low + 4 * rows), moved, 0.0)

    def group(first):
        mine = yours = 0.0
        for i in range(2):
            mine += placed(own, first + i, 32 * i, 0, 4, 2 - 2 * ta)
            mine += placed(zo, first + i, 32 * i, 2 - 2 * ta, 2, 4 * ta)
            yours += placed(par, first + i, 32 * i, 0, 4, 2 - 2 * ta)
            yours += placed(zp, first + i, 32 * i, 2 - 2 * ta, 2, 4 * ta)
        g0, g1 = (mine, yours) if ta == 0 else (yours, mine)
        return g0 + pltpu.roll(g1, 64, 1)

    def caches(slot):
        out = placed(own, slot, 32 * ta, 0, 4, 2 - 2 * ta)
        out += placed(zo, slot, 32 * ta, 2 - 2 * ta, 2, 4 * ta)
        out += placed(par, slot, 32 * other, 0, 4, 2 - 2 * ta)
        return out + placed(zp, slot, 32 * other, 2 - 2 * ta, 2, 4 * ta)

    def edge_products(w, low, high, order, last=False):
        pieces = []
        for t, a in order:
            s = 32 * t + 4 * a
            if s == 0:
                pieces.append(low.astype(bf16))
                continue
            joined = jnp.where(lane < s, 0.0 if high is None else high, low)
            pieces.append(pltpu.roll(joined, 128 - s, 1).astype(bf16))
        stacked = jnp.concatenate(pieces, axis=0)
        if last:
            outer = jnp.concatenate([w[:channels, :], w[2 * channels :, :]], axis=0)
            p = jnp.dot(outer, stacked, preferred_element_type=f32)
            return jnp.where(column == 2, p[:channels], p[channels:])
        p = jnp.dot(w[...], stacked, preferred_element_type=f32)
        p0, p1, p2 = (p[b * channels : (b + 1) * channels] for b in range(3))
        across = jnp.where(column == 2, p0, p2)
        own_part = jnp.where(column == 2, pltpu.roll(p0, 127, 1), pltpu.roll(p2, 1, 1)) + p1
        return across, own_part

    def to_edges(p, edge_ref, q):
        moved = pltpu.roll(jnp.where(lane == 0, p[2], p[0]), q + 2, 1)
        here = (lane == q + 1) | (lane == q + 2)
        edge_ref[...] = edge_ref[...] + jnp.where(here, moved, 0.0)

    def first_products(f, pair):
        forward = PV[0, f, pair] if f < 2 else product(w1[...], A, (), f, 2 * pair, forward_order)
        gradient = PV[1, f - 2, pair] if f > 1 else product(w2f[...], C, (), f, 2 * pair, gradient_taps(f))
        return parts(forward), parts(gradient)

    partial_products(ws, AC, PV, other)
    act_edges = pltpu.roll(act(group(0), gin), 64, 1)
    cin_edges = caches(4)
    across, own_part = edge_products(
        w1, jnp.where(lane < 64, cin_edges, act_edges), jnp.where(lane < 64, act_edges, 0.0),
        forward_order,
    )
    PA[...] = across
    EA[...] = own_part
    across, own_part = edge_products(w2f, group(2), None, gradient_order)
    PC[...] = across
    EC[...] = own_part
    cmid_edges = pltpu.roll(caches(5), 124, 1)

    def first_layer(f):
        for pair in range(2):
            pf, pb = first_products(f, pair)
            for i in range(2):
                e = 2 * pair + i
                q = f * 32 + e * 4
                hidden = (shifted_sum(pf[i], PA, q) + bin_).astype(bf16).astype(f32)
                back = shifted_sum(pb[i], PC, q)
                to_edges(pf[i], EA, q)
                to_edges(pb[i], EC, q)
                a, d = act_and_back(hidden, gmid, back)
                if e == 0:
                    a = jnp.where(first_row, a, 0.0)
                    d = jnp.where(first_row, d, 0.0)
                if e == 3:
                    a = jnp.where(last_row, a, 0.0)
                    d = jnp.where(last_row, d, 0.0)
                M[2 + f, e] = a.astype(bf16)
                D[f, e] = d.astype(bf16)

    for f in range(4):
        first_layer(f)

    late = [second_products(2 * other, M, D, w2, w1f)]
    hidden = (EA[...] + bin_).astype(bf16).astype(f32)
    a, d = act_and_back(hidden, gmid, EC[...])
    row = (lane % 32) // 4
    inside = ((column == 2) & left_col) | ((column == 1) & right_col)
    inside = inside & (row < 4) & ((row > 0) | first_row) & ((row < 3) | last_row)
    a = jnp.where(inside, a, 0.0).astype(bf16).astype(f32)
    d = jnp.where(inside, d, 0.0).astype(bf16).astype(f32)
    a = pltpu.roll(a, 64, 1)
    low = jnp.where(lane < 64, cmid_edges, a)
    PA[...] = edge_products(w2, low, jnp.where(lane < 64, a, 0.0), forward_order, last=True)
    PC[...] = edge_products(w1f, d, None, gradient_order, last=True)
    late.append(second_products(2 * other + 1, M, D, w2, w1f))

    for slot in range(2):
        second_layer(2 * other + slot, sp, slot, send, late[slot], PA, PC, vec, False)


def assemble_body(keep, got, m1, dec, grad, scr):
    channels = keep.shape[3]
    flat = 4 * channels
    ta = lax.axis_index("ta")
    for f in range(2):
        for i in range(2):
            mine = pl.ds(f * flat + 2 * ta + i, channels, stride=4)
            yours = pl.ds(f * flat + 2 - 2 * ta + i, channels, stride=4)
            scr[mine, :] = keep[0, f, i]
            grad[mine, :] = keep[1, f, i]
            scr[yours, :] = got[0, f, i].astype(f32)
            grad[yours, :] = m1[4 + 2 * f + i].astype(f32) + got[1, f, i].astype(f32)
    dec[...] = scr[...].astype(bf16)


def per_device(
    frames, cache_in, cache_mid, gain_in, gain_mid,
    weight_in, bias_in, weight_mid, bias_mid, cotangent,
):
    n, c, height, width = frames.shape
    flat = lambda v: v.reshape(n * c * height, width)
    tile = (c, width)
    limit = lambda mib: pltpu.CompilerParams(vmem_limit_bytes=mib << 20)
    row = lambda v: v.reshape(1, c)
    taps = lambda w: w.reshape(3, 3 * c, 3 * c)
    ed, scr, wm, rows = pl.pallas_call(
        fetch_body,
        in_specs=[HB] * 9,
        out_specs=(VM,) * 4,
        out_shape=(
            pltpu.VMEM(tile, bf16),
            pltpu.VMEM((8, c * height, width), f32),
            pltpu.VMEM((3, 3 * c, 3 * c), bf16),
            pltpu.VMEM((4, 1, c), f32),
        ),
        scratch_shapes=[
            pltpu.VMEM((8, c * height, width), bf16),
            pltpu.SemaphoreType.DMA((16,)),
            pltpu.SemaphoreType.DMA((5,)),
        ],
        compiler_params=limit(6),
        name="fetch",
    )(
        *far(
            flat(frames), flat(cotangent), flat(cache_in), flat(cache_mid),
            taps(weight_mid), row(gain_in), row(gain_mid), row(bias_in), row(bias_mid),
        )
    )
    m1, m2, oc, sw = pl.pallas_call(
        pack_body,
        in_specs=[VM],
        out_specs=(VM,) * 4,
        out_shape=(
            pltpu.VMEM((12,) + tile, bf16),
            pltpu.VMEM((12,) + tile, bf16),
            pltpu.VMEM((2, 4) + tile, bf16),
            pltpu.VMEM((17,) + tile, bf16),
        ),
        compiler_params=limit(4),
        name="pack",
    )(*near(scr))

    wide = lax.axis_size("wa")
    high = lax.axis_size("ha")
    pairs = lambda start: [
        p for i in range(start, wide - 1, 2) for p in ((i, i + 1), (i + 1, i))
    ]
    one = [(2 * i, 2 * i + 2) for i in range(high - 1)]
    one += [(2 * i + 3, 2 * i + 1) for i in range(high - 1)]
    two = [(2 * i + 2, 2 * i + 1) for i in range(high - 1)]
    two += [(2 * i + 1, 2 * i + 2) for i in range(high - 1)]
    second = lax.ppermute(ed, "wa", pairs(1))
    first = lax.ppermute(ed, "wa", pairs(0))
    z1 = lax.ppermute(m1, ("ha", "ta"), one)
    z2 = lax.ppermute(m2, ("ha", "ta"), two)
    sw, edge = pl.pallas_call(
        merge_body,
        in_specs=[VM] * 3,
        out_specs=(VM,) * 2,
        out_shape=(pltpu.VMEM((17,) + tile, bf16), pltpu.VMEM(tile, bf16)),
        input_output_aliases={2: 0},
        compiler_params=limit(2),
        name="merge",
    )(*near(first, second, sw))
    sp = lax.ppermute(sw, "ta", [(0, 1), (1, 0)])
    e1 = lax.ppermute(edge, ("ha", "ta"), one)
    e2 = lax.ppermute(edge, ("ha", "ta"), two)

    matrix = pltpu.VMEM((3 * c, 9 * c), bf16)
    ws, w2, w1f, vec = pl.pallas_call(
        weights_body,
        in_specs=[VM] * 3 + [pl.BlockSpec(memory_space=pl.ANY)],
        out_specs=(VM,) * 4,
        out_shape=(
            pltpu.VMEM((2, 3 * c, 9 * c), bf16),
            matrix,
            matrix,
            pltpu.VMEM((4,) + tile, f32),
        ),
        compiler_params=limit(8),
        name="weights",
    )(*near(taps(weight_in), wm, rows), m2)
    staged = (
        pltpu.VMEM((2, 6, 6) + tile, bf16),
        pltpu.VMEM((6, 4) + tile, bf16),
        pltpu.VMEM((2, 2, 2, 3 * c, 2 * width), f32),
    )
    AC, M, PV = pl.pallas_call(
        per_core(lead_body),
        in_specs=[VM] * 7,
        out_specs=(VM,) * 3,
        out_shape=staged,
        compiler_params=limit(8),
        name="lead",
    )(*near(m1, m2, oc, z1, z2, vec, ws))
    half = pltpu.VMEM((2, 2, 2) + tile, f32)
    AC, M, PV, D, PA, PC, send = pl.pallas_call(
        per_core(main_body),
        in_specs=[VM] * 11,
        out_specs=(VM,) * 7,
        out_shape=staged
        + (
            pltpu.VMEM((6, 4) + tile, bf16),
            pltpu.VMEM(tile, f32),
            pltpu.VMEM(tile, f32),
            pltpu.VMEM((2, 2, 2) + tile, bf16),
        ),
        scratch_shapes=[pltpu.VMEM(tile, f32), pltpu.VMEM(tile, f32)],
        input_output_aliases={0: 0, 1: 1, 2: 2},
        compiler_params=limit(12),
        name="block",
    )(*near(AC, M, PV, sp, edge, e1, e2, ws, w2, w1f, vec))
    got = lax.ppermute(send, "ta", [(0, 1), (1, 0)])
    keep = pl.pallas_call(
        per_core(own_body),
        in_specs=[VM] * 8,
        out_specs=VM,
        out_shape=half,
        compiler_params=limit(8),
        name="own",
    )(*near(m2, M, D, PA, PC, w2, w1f, vec))
    decoded, grad = pl.pallas_call(
        assemble_body,
        in_specs=[VM] * 3,
        out_shape=(
            jax.ShapeDtypeStruct((n * c * height, width), bf16),
            jax.ShapeDtypeStruct((n * c * height, width), f32),
        ),
        scratch_shapes=[pltpu.VMEM((n * c * height, width), f32)],
        compiler_params=limit(8),
        name="assemble",
    )(*near(keep, got, m1))
    return decoded.reshape(frames.shape), grad.reshape(frames.shape)


def solution(mesh):
    split = P(("grp", "ta"), None, "ha", "wa")
    cache = P("grp", None, "ha", "wa")
    return jax.shard_map(
        per_device,
        mesh=mesh,
        in_specs=(split, cache, cache, P(), P(), P(), P(), P(), P(), split),
        out_specs=(split, split),
        check_vma=False,
    )
```
